128 devices in a mesh: probe: 4 (over z_hi, core), fsdp: 32 (over y, z_lo, x).
Axes of the slice: x: 4, y: 4, z: 4 (z_hi: 2, z_lo: 2; z = z_hi * 2 + z_lo), core: 2. Of those that a mesh axis runs over, the one named last changes fastest.
Arguments:
- hidden: bfloat16 [65536, 2048], P(('probe', 'fsdp')), may hold values from -6 to 6
- norm_gain: bfloat16 [2048], replicated, may hold values from 0.5 to 1.5
- query_weight: bfloat16 [2048, 2048], P('fsdp'), may hold values from -1 to 1
- key_weight: bfloat16 [2048, 512], P('fsdp'), may hold values from -16 to 16
- value_weight: bfloat16 [2048, 512], P('fsdp'), may hold values from -0.125 to 0.125
- output_weight: bfloat16 [2048, 2048], P('fsdp'), may hold values from -0.125 to 0.125
- probe_seed: int32 [4], P('probe'), may hold values from 0 to 1073741823
Outputs:
- curvature_value: float32 [2048, 512], P('fsdp', 'probe')
- curvature_output: float32 [2048, 2048], P('fsdp', 'probe')
The draws below stay inside these ranges and needn't reach their ends.
All inputs are finite; a program needn't handle non-finite values.
Results may differ from the reference program's by a relative error of at most 0.024.
Values may be sent and summed in bfloat16 or wider, within the bound.
A program may use at most 128 MiB of HBM per device.

```python
import jax
import jax.numpy as jnp
from jax import lax

D = 2048
HEADS = 16
KV_HEADS = 4
HEAD_DIM = 128
SEQ = 256
TOK_DEV = 512
QW = 2048
KW = 512
TOKENS = 65536
N_PROBE = 4
N_FSDP = 32


def query_base(key):
    normals = jax.random.normal(jax.random.fold_in(key, 7101), (D, HEADS * HEAD_DIM), jnp.float32)
    return jnp.clip(normals, -6.0, 6.0) * D ** (-0.5)


def draw_query_weight(key, part):
    return query_base(key).astype(jnp.bfloat16)


def draw_key_weight(key, part):
    normals = jax.random.normal(jax.random.fold_in(key, 7102), (D, KV_HEADS * HEAD_DIM), jnp.float32)
    noise_part = jnp.clip(normals, -6.0, 6.0) * D ** (-0.5)
    return noise_part.astype(jnp.bfloat16)


def touch_ends(entries, own_key, least, largest):
    longest = entries.shape.index(max(entries.shape))
    spots = []
    for shift in (0, 1):
        where = [jax.random.randint(jax.random.fold_in(own_key, axis), (), 0, length) for axis, length in enumerate(entries.shape)]
        where[longest] = (where[longest] + shift) % entries.shape[longest]
        spots.append(tuple(where))
    return entries.at[spots[0]].set(least).at[spots[1]].set(largest)


def block_scale(stream_key, extent, split, smallest, largest):
    factor_of = 1.0
    for axis_at, blocks in split:
        draws = jax.random.uniform(jax.random.fold_in(jax.random.fold_in(stream_key, 6), axis_at), (blocks,), jnp.float32, smallest / len(split), largest / len(split))
        factor_of = factor_of * jnp.repeat(jnp.exp(draws), extent[axis_at] // blocks).reshape((-1,) + (1,) * (len(extent) - 1 - axis_at))
    return factor_of


def gaussian(stream_key, shape, scale, bound, split=(), kind=jnp.bfloat16):
    factor_of = block_scale(stream_key, shape, split, -0.22, 0.18) if split else 1.0
    values = jax.random.normal(stream_key, shape, jnp.float32) * scale * factor_of
    return jnp.minimum(jnp.maximum(values, -bound), bound).astype(kind)


def setup_inputs(seed: int = 0) -> dict:
    seeds = jax.random.split(jax.random.key(seed), 8)
    return {
        "hidden": gaussian(seeds[0], (TOKENS, D), 1.0, 6.0, ((0, 128),)),
        "norm_gain": jnp.clip(1.0 + 0.1 * jax.random.normal(seeds[1], (D,), jnp.float32), 0.5, 1.5).astype(jnp.bfloat16),
        "query_weight": draw_query_weight(jax.random.fold_in(seeds[7], 71), 0),
        "key_weight": draw_key_weight(jax.random.fold_in(seeds[7], 71), 0),
        "value_weight": gaussian(seeds[4], (D, KW), D ** -0.5, 0.125, ((0, 32),)),
        "output_weight": gaussian(seeds[5], (QW, D), QW ** -0.5, 0.125, ((0, 32),)),
        "probe_seed": touch_ends(jax.random.randint(seeds[6], (N_PROBE,), 0, 1073741824), jax.random.fold_in(seeds[6], 1), 0, 1073741823).astype(jnp.int32),
    }


norm_eps = 1e-05
rope_base = 500000.0

def sign_table(seed_value, matrix_code, row_total, column_total):
    row_index = lax.broadcasted_iota(jnp.int32, (row_total, column_total), 0)
    column_index = lax.broadcasted_iota(jnp.int32, (row_total, column_total), 1)
    hashed = (row_index * column_total + column_index) * 747796405 + (seed_value * 1664525 + matrix_code * 374761393)
    hashed = hashed ^ lax.shift_right_logical(hashed, jnp.int32(15))
    hashed = hashed * 668265261
    hashed = hashed ^ lax.shift_right_logical(hashed, jnp.int32(13))
    hashed = hashed * 1274126177
    hashed = hashed ^ lax.shift_right_logical(hashed, jnp.int32(16))
    return jnp.where(hashed & 1 == 1, 1.0, -1.0).astype(jnp.bfloat16)

def normalize(rows_in, gain_row):
    values = rows_in.astype(jnp.float32)
    inverse = lax.rsqrt(lax.optimization_barrier(jnp.mean(values * values, axis=1, keepdims=True)) + norm_eps)
    return (values * inverse * gain_row.astype(jnp.float32)[None, :]).astype(jnp.bfloat16)

def rotate(projected, head_count):
    row_count = projected.shape[0]
    columns = projected.shape[1]
    head_size = columns // head_count
    half_dim = head_size // 2
    position = (lax.broadcasted_iota(jnp.int32, (row_count, 1), 0) % SEQ).astype(jnp.float32)
    exponent = lax.broadcasted_iota(jnp.int32, (1, half_dim), 1).astype(jnp.float32) * (-2.0 / head_size)
    frequency = jnp.power(jnp.float32(rope_base), exponent)
    angles = position * frequency
    cosine = jnp.cos(angles)[:, None, :]
    sine_part = jnp.sin(angles)[:, None, :]
    shaped = projected.reshape(row_count, head_count, head_size)
    leading = shaped[:, :, :half_dim]
    trailing = shaped[:, :, half_dim:]
    turned = jnp.concatenate([leading * cosine - trailing * sine_part, trailing * cosine + leading * sine_part], axis=2)
    return turned.reshape(row_count, columns).astype(jnp.bfloat16)

def attend(query_rows, key_rows):
    row_count = query_rows.shape[0]
    key_heads = key_rows.shape[1] // HEAD_DIM
    group_size = query_rows.shape[1] // key_rows.shape[1]
    sequences = row_count // SEQ
    grouped_query = query_rows.reshape(sequences, SEQ, key_heads, group_size, HEAD_DIM).astype(jnp.float32)
    grouped_key = key_rows.reshape(sequences, SEQ, key_heads, HEAD_DIM).astype(jnp.float32)
    scores = jnp.einsum('bqkgd,bskd->bkgqs', grouped_query, grouped_key) * HEAD_DIM ** (-0.5)
    causal_mask = lax.broadcasted_iota(jnp.int32, (SEQ, SEQ), 0) >= lax.broadcasted_iota(jnp.int32, (SEQ, SEQ), 1)
    scores = jnp.where(causal_mask, scores, -1e+30)
    highest = lax.optimization_barrier(jnp.max(scores, axis=4, keepdims=True))
    raised = jnp.exp(scores - highest)
    return (raised / lax.optimization_barrier(jnp.sum(raised, axis=4, keepdims=True))).astype(jnp.bfloat16)

def mix_values(attention, value_rows):
    sequences = attention.shape[0]
    key_heads = attention.shape[1]
    group_size = attention.shape[2]
    grouped_value = value_rows.reshape(sequences, SEQ, key_heads, HEAD_DIM).astype(jnp.float32)
    combined = jnp.einsum('bkgqs,bskd->bqkgd', attention.astype(jnp.float32), grouped_value)
    return combined.reshape(sequences * SEQ, key_heads * group_size * HEAD_DIM)

def spread_back(attention, upstream):
    sequences = attention.shape[0]
    key_heads = attention.shape[1]
    group_size = attention.shape[2]
    grouped_upstream = upstream.reshape(sequences, SEQ, key_heads, group_size, HEAD_DIM).astype(jnp.float32)
    spread = jnp.einsum('bkgqs,bqkgd->bskd', attention.astype(jnp.float32), grouped_upstream)
    return spread.reshape(sequences * SEQ, key_heads * HEAD_DIM)

def device_terms(rows_in, norm_gain, query_weight, key_weight, value_weight, output_weight, seed_value):
    normed = normalize(rows_in, norm_gain)
    query_rows = rotate(jnp.dot(normed, query_weight, preferred_element_type=jnp.float32), HEADS)
    key_rows = rotate(jnp.dot(normed, key_weight, preferred_element_type=jnp.float32), KV_HEADS)
    value_rows = jnp.dot(normed, value_weight, preferred_element_type=jnp.float32).astype(jnp.bfloat16)
    attention = attend(query_rows, key_rows)
    context = mix_values(attention, value_rows).astype(jnp.bfloat16)
    signs_value = sign_table(seed_value, 0, D, KW)
    signs_out = sign_table(seed_value, 1, QW, D)
    tangent_value = (jnp.dot(normed, signs_value, preferred_element_type=jnp.float32) * D ** (-0.5)).astype(jnp.bfloat16)
    tangent_context = mix_values(attention, tangent_value).astype(jnp.bfloat16)
    forward_part = jnp.dot(tangent_context, output_weight, preferred_element_type=jnp.float32)
    probe_part = jnp.dot(context, signs_out, preferred_element_type=jnp.float32) * QW ** (-0.5)
    cotangent = (forward_part + probe_part).astype(jnp.bfloat16)
    back_context = jnp.dot(cotangent, output_weight.T, preferred_element_type=jnp.float32).astype(jnp.bfloat16)
    back_value = spread_back(attention, back_context).astype(jnp.bfloat16)
    term_value = jnp.dot(normed.T, back_value, preferred_element_type=jnp.float32)
    term_out = jnp.dot(context.T, cotangent, preferred_element_type=jnp.float32)
    return (term_value, term_out)

def reference(hidden, norm_gain, query_weight, key_weight, value_weight, output_weight, probe_seed):
    blocks = N_PROBE * N_FSDP

    def one_block(totals, block_index):
        rows_in = lax.dynamic_slice_in_dim(hidden, block_index * TOK_DEV, TOK_DEV, 0)
        seed_value = probe_seed[block_index // N_FSDP]
        term_value, term_out = device_terms(rows_in, norm_gain, query_weight, key_weight, value_weight, output_weight, seed_value)
        rounded_value = lax.optimization_barrier(term_value.astype(jnp.bfloat16))
        rounded_out = lax.optimization_barrier(term_out.astype(jnp.bfloat16))
        return ((totals[0] + rounded_value.astype(jnp.float32), totals[1] + rounded_out.astype(jnp.float32)), None)
    starting = (jnp.zeros((D, KW), jnp.float32), jnp.zeros((QW, D), jnp.float32))
    totals, unused = lax.scan(one_block, starting, jnp.arange(blocks, dtype=jnp.int32))
    return (totals[0], totals[1])
```

```python
import functools

import jax
import jax.numpy as jnp
from jax import lax
from jax.experimental import pallas as pl
from jax.experimental.pallas import tpu as pltpu
from jax.sharding import PartitionSpec as P

MESH = pl.DeviceIdType.MESH
HEAD_DIM = 128
SEQ = 256
norm_eps = 1e-05
rope_base = 500000.0
ORDERS = (("z", "x", "y"), ("x", "y", "z"), ("z", "y", "x"), ("y", "x", "z"))


class Place:
    def __init__(self):
        p = lax.axis_index("probe")
        f = lax.axis_index("fsdp")
        self.p, self.f = p, f
        self.x = lax.rem(f, 4)
        self.zl = lax.rem(lax.div(f, 4), 2)
        self.y = lax.div(f, 8)
        self.zh = lax.div(p, 2)
        self.c = lax.rem(p, 2)
        self.z = self.zh * 2 + self.zl

    def move(self, axis, step):
        x, y, z = self.x, self.y, self.z
        if axis == "x":
            x = lax.rem(x + step + 4, 4)
        elif axis == "y":
            y = lax.rem(y + step + 4, 4)
        else:
            z = lax.rem(z + step + 4, 4)
        return (lax.div(z, 2) * 2 + self.c, y * 8 + lax.rem(z, 2) * 4 + x)

    def partner(self):
        return (self.zh * 2 + 1 - self.c, self.f)

    def neighbours(self):
        return [self.move(a, s) for a in ("x", "y", "z") for s in (1, -1)] + [self.partner()]


def meet(place):
    barrier = pltpu.get_barrier_semaphore()
    peers = place.neighbours()
    for peer in peers:
        pl.semaphore_signal(barrier, inc=1, device_id=peer, device_id_type=MESH)
    pl.semaphore_wait(barrier, len(peers))


class Copies:
    def __init__(self, send_sems, recv_sems):
        self.send_sems, self.recv_sems = send_sems, recv_sems
        self.used = 0
        self.started = []

    def slot(self):
        self.used += 1
        return self.used - 1

    def send(self, slot, ref, peer, dst=None):
        copy = pltpu.make_async_remote_copy(
            src_ref=ref,
            dst_ref=ref if dst is None else dst,
            send_sem=self.send_sems.at[slot],
            recv_sem=self.recv_sems.at[slot],
            device_id=peer,
            device_id_type=MESH,
        )
        copy.start()
        self.started.append(copy)

    def wait_recv(self, slot, ref, peer):
        pltpu.make_async_remote_copy(
            src_ref=ref,
            dst_ref=ref,
            send_sem=self.send_sems.at[slot],
            recv_sem=self.recv_sems.at[slot],
            device_id=peer,
            device_id_type=MESH,
        ).wait_recv()

    def finish(self):
        for copy in self.started:
            copy.wait_send()


def gather_steps(buf, order, place, copies):
    both = slice(None)

    def region(have, where, core, halves):
        def pick(axis, extent):
            return pl.ds(0, extent) if axis in have else pl.ds(where[axis], 1)

        return buf.at[pick("y", 4), pick("z", 2), pick("x", 4), core, halves]

    here = {"x": place.x, "y": place.y, "z": place.zl}
    core, other = place.c, 1 - place.c
    partner = place.partner()
    from_partner = []

    def share(have, where):
        slot = copies.slot()
        copies.send(slot, region(have, where, core, pl.ds(0, 2)), partner)
        from_partner.append((slot, region(have, where, other, pl.ds(0, 2))))

    have = ()
    for phase, axis in enumerate(order):
        last = phase == 2
        if last:
            share(have, here)
        if axis == "z":
            slots = (copies.slot(), copies.slot())
            for half, step in ((0, 1), (1, -1)):
                copies.send(
                    slots[half], region(have, here, core, pl.ds(half, 1)), place.move("z", step)
                )
            yield
            there = dict(here, z=1 - place.zl)
            for half, step in ((0, -1), (1, 1)):
                copies.wait_recv(
                    slots[half], region(have, there, core, pl.ds(half, 1)), place.move("z", step)
                )
            if last:
                share(have, there)
        else:
            at = {s: dict(here, **{axis: lax.rem(here[axis] + s + 4, 4)}) for s in (-1, 1, 2)}
            up, down, up2, down2 = (copies.slot() for _ in range(4))
            ahead, behind = place.move(axis, 1), place.move(axis, -1)
            copies.send(up, region(have, here, core, pl.ds(0, 2)), ahead)
            copies.send(down, region(have, here, core, pl.ds(0, 2)), behind)
            yield
            copies.wait_recv(up, region(have, at[-1], core, pl.ds(0, 2)), behind)
            copies.send(up2, region(have, at[-1], core, pl.ds(0, 1)), ahead)
            copies.wait_recv(down, region(have, at[1], core, pl.ds(0, 2)), ahead)
            copies.send(down2, region(have, at[1], core, pl.ds(1, 1)), behind)
            if last:
                share(have, at[-1])
                share(have, at[1])
            yield
            copies.wait_recv(up2, region(have, at[2], core, pl.ds(0, 1)), behind)
            copies.wait_recv(down2, region(have, at[2], core, pl.ds(1, 1)), ahead)
            if last:
                share(have, at[2])
        have = have + (axis,)
    yield
    for slot, ref in from_partner:
        copies.wait_recv(slot, ref, partner)


def in_turn(walks):
    walks = list(walks)
    while walks:
        left = []
        for walk in walks:
            try:
                next(walk)
                left.append(walk)
            except StopIteration:
                pass
        walks = left


def gather_kernel(wq, wk, wv, wo, qkv_out, out_out, qkv, out, send_sems, recv_sems, load_sems, store_sems):
    place = Place()
    loads = []

    def load(src, dst):
        copy = pltpu.make_async_copy(src, dst, load_sems.at[len(loads)])
        copy.start()
        loads.append(copy)

    def own(buf, columns):
        return buf.at[place.y, place.zl, place.x, place.c, :, :, columns]

    def rows(w, columns):
        return w.at[place.c, :, :, columns]

    for h in range(4):
        load(rows(wq, pl.ds(h * 512, 512)), own(qkv.at[h], pl.ds(0, 512)))
        load(rows(wk, pl.ds(h * 128, 128)), own(qkv.at[h], pl.ds(512, 128)))
        load(rows(wv, pl.ds(h * 128, 128)), own(qkv.at[h], pl.ds(640, 128)))
    for j in range(4):
        load(rows(wo, pl.ds(j * 512, 512)), own(out.at[j], pl.ds(0, 512)))
    meet(place)
    for copy in loads:
        copy.wait()
    copies = Copies(send_sems, recv_sems)
    in_turn([gather_steps(qkv.at[h], ORDERS[h], place, copies) for h in range(4)]+[gather_steps(out.at[h], ORDERS[h], place, copies) for h in range(4)])
    stores = [
        pltpu.make_async_copy(qkv, qkv_out, store_sems.at[0]),
        pltpu.make_async_copy(out, out_out, store_sems.at[1]),
    ]
    for copy in stores:
        copy.start()
    copies.finish()
    for copy in stores:
        copy.wait()


def gather_all(wq, wk, wv, wo):
    halves = [w.reshape(2, 2, 16, w.shape[1]) for w in (wq, wk, wv, wo)]
    shapes = [(4, 4, 2, 4, 2, 2, 16, 768), (4, 4, 2, 4, 2, 2, 16, 512)]
    copies = 120
    qkv, out = pl.pallas_call(
        gather_kernel,
        out_shape=[jax.ShapeDtypeStruct(s, jnp.bfloat16) for s in shapes],
        in_specs=[pl.BlockSpec(memory_space=pl.ANY)] * 4,
        out_specs=[pl.BlockSpec(memory_space=pl.ANY)] * 2,
        scratch_shapes=[pltpu.VMEM(s, jnp.bfloat16) for s in shapes]
        + [
            pltpu.SemaphoreType.DMA((copies,)),
            pltpu.SemaphoreType.DMA((copies,)),
            pltpu.SemaphoreType.DMA((16,)),
            pltpu.SemaphoreType.DMA((2,)),
        ],
        compiler_params=pltpu.CompilerParams(
            collective_id=0, has_side_effects=True, vmem_limit_bytes=48 * 1024 * 1024
        ),
    )(*halves)
    return qkv.reshape(4, 2048, 768), out.reshape(4, 2048, 512)


REDUCE_ORDERS = (("x", "y", "z"), ("y", "z", "x"), ("x", "z", "y"), ("y", "x", "z"), ("z", "x", "y"))


def wide(value):
    return value.astype(jnp.float32)


def reduce_steps(unit, order, mine, theirs, landing, result, place, copies, partner_slot):
    here = {"x": place.x, "y": place.y, "z": place.z}

    def region(done, where, half):
        at = dict(where)

        def pick(axis, extent):
            return pl.ds(at[axis], 1) if axis in done else pl.ds(0, extent)

        if "z" in done:
            zh, zl = pl.ds(lax.div(at["z"], 2), 1), pl.ds(lax.rem(at["z"], 2), 1)
        else:
            zh, zl = pl.ds(0, 2), pl.ds(0, 2)
        return mine.at[zh, pick("y", 4), zl, pick("x", 4), half]

    copies.wait_recv(partner_slot, theirs, place.partner())

    def add_partner(i, carry):
        zh, y = lax.div(i, 4), lax.rem(i, 4)
        mine[zh, y] = (wide(mine[zh, y]) + wide(theirs[zh, y])).astype(jnp.bfloat16)
        return carry

    lax.fori_loop(0, 8, add_partner, 0)
    done = ()
    for stage, axis in enumerate(order):
        land = landing[stage]
        done = done + (axis,)
        at = {s: dict(here, **{axis: lax.rem(here[axis] + s + 4, 4)}) for s in (-1, 0, 1, 2)}
        ahead, behind = place.move(axis, 1), place.move(axis, -1)
        slots = [copies.slot() for _ in range(6)]

        def send(slot, step, half, peer):
            copies.send(slots[slot], region(done, at[step], half), peer, dst=land.at[slot])

        def wait(slot, peer):
            copies.wait_recv(slots[slot], land.at[slot], peer)

        send(0, 2, 0, ahead)
        send(1, 2, 1, behind)
        send(3, 1, 1, ahead)
        send(4, -1, 0, behind)
        yield
        for slot, step, half, source, peer, onward in (
            (0, 1, 0, behind, ahead, 2),
            (1, -1, 1, ahead, behind, 5),
        ):
            wait(slot, source)
            part = region(done, at[step], half)
            part[...] = (wide(part[...]) + wide(land[slot])).astype(jnp.bfloat16)
            send(onward, step, half, peer)
        yield
        for slot, source in ((3, behind), (4, ahead), (2, behind), (5, ahead)):
            wait(slot, source)
        for half in (0, 1):
            part = region(done, at[0], half)
            total = wide(part[...]) + wide(land[2 + half]) + wide(land[4 + half])
            if stage == 2:
                result[pl.ds(32 * half, 32), :] = total.reshape(32, 128)
            else:
                part[...] = total.astype(jnp.bfloat16)


def stage_shape(order, stage):
    done = order[: stage + 1]
    z = 1 if "z" in done else 2
    return (6, z, 1 if "y" in done else 4, z, 1 if "x" in done else 4, 32, 128)


def reduce_kernel(term_value, term_out, value_ref, out_ref, mine, theirs, *rest):
    landing, (send_sems, recv_sems, load_sems) = rest[:15], rest[15:]
    place = Place()
    copies = Copies(send_sems, recv_sems)

    def columns(unit, core):
        ref = term_value if unit == 4 else term_out
        start = 0 if unit == 4 else unit * 128
        return ref.at[:, core, :, :, :, :, :, pl.ds(start, 128)]

    loads = []
    for unit in range(5):
        copy = pltpu.make_async_copy(columns(unit, place.c), mine.at[unit], load_sems.at[unit])
        copy.start()
        loads.append(copy)
    meet(place)
    slots = []
    for unit in range(5):
        slots.append(copies.slot())
        copies.send(slots[-1], columns(unit, 1 - place.c), place.partner(), dst=theirs.at[unit])
    for copy in loads:
        copy.wait()
    in_turn(
        reduce_steps(
            unit,
            REDUCE_ORDERS[unit],
            mine.at[unit],
            theirs.at[unit],
            landing[3 * unit : 3 * unit + 3],
            value_ref if unit == 4 else out_ref.at[:, pl.ds(128 * unit, 128)],
            place,
            copies,
            slots[unit],
        )
        for unit in range(5)
    )
    copies.finish()


def reduce_all(term_value, term_out):
    table = (2, 4, 2, 4, 2, 32, 128)
    operands = [t.reshape(2, 2, 4, 2, 4, 2, 32, t.shape[2]) for t in (term_value, term_out)]
    copies = 5 + 5 * 18
    return pl.pallas_call(
        reduce_kernel,
        out_shape=[
            jax.ShapeDtypeStruct((64, 128), jnp.float32),
            jax.ShapeDtypeStruct((64, 512), jnp.float32),
        ],
        in_specs=[pl.BlockSpec(memory_space=pl.ANY)] * 2,
        out_specs=[pl.BlockSpec(memory_space=pltpu.VMEM)] * 2,
        scratch_shapes=[pltpu.VMEM((5,) + table, jnp.bfloat16)] * 2
        + [
            pltpu.VMEM(stage_shape(REDUCE_ORDERS[unit], stage), jnp.bfloat16)
            for unit in range(5)
            for stage in range(3)
        ]
        + [
            pltpu.SemaphoreType.DMA((copies,)),
            pltpu.SemaphoreType.DMA((copies,)),
            pltpu.SemaphoreType.DMA((5,)),
        ],
        compiler_params=pltpu.CompilerParams(
            collective_id=1, has_side_effects=True, vmem_limit_bytes=48 * 1024 * 1024
        ),
    )(*operands)


def sign_table(seed_value, matrix_code, row_total, column_total):
    row_index = lax.broadcasted_iota(jnp.int32, (row_total, column_total), 0)
    column_index = lax.broadcasted_iota(jnp.int32, (row_total, column_total), 1)
    hashed = (row_index * column_total + column_index) * 747796405 + (
        seed_value * 1664525 + matrix_code * 374761393
    )
    hashed = hashed ^ lax.shift_right_logical(hashed, jnp.int32(15))
    hashed = hashed * 668265261
    hashed = hashed ^ lax.shift_right_logical(hashed, jnp.int32(13))
    hashed = hashed * 1274126177
    hashed = hashed ^ lax.shift_right_logical(hashed, jnp.int32(16))
    return jnp.where(hashed & 1 == 1, 1.0, -1.0).astype(jnp.bfloat16)


def normalize(rows_in, gain_row):
    values = rows_in.astype(jnp.float32)
    inverse = lax.rsqrt(jnp.mean(values * values, axis=1, keepdims=True) + norm_eps)
    return (values * inverse * gain_row.astype(jnp.float32)[None, :]).astype(jnp.bfloat16)


def rotate(projected, head_count):
    row_count = projected.shape[0]
    columns = projected.shape[1]
    head_size = columns // head_count
    half_dim = head_size // 2
    position = (lax.broadcasted_iota(jnp.int32, (row_count, 1), 0) % SEQ).astype(jnp.float32)
    exponent = lax.broadcasted_iota(jnp.int32, (1, half_dim), 1).astype(jnp.float32) * (
        -2.0 / head_size
    )
    frequency = jnp.power(jnp.float32(rope_base), exponent)
    angles = position * frequency
    cosine = jnp.cos(angles)[:, None, :]
    sine_part = jnp.sin(angles)[:, None, :]
    shaped = projected.reshape(row_count, head_count, head_size)
    leading = shaped[:, :, :half_dim]
    trailing = shaped[:, :, half_dim:]
    turned = jnp.concatenate(
        [leading * cosine - trailing * sine_part, trailing * cosine + leading * sine_part], axis=2
    )
    return turned.reshape(row_count, columns).astype(jnp.bfloat16)


def attend(query_rows, key_rows):
    row_count = query_rows.shape[0]
    key_heads = key_rows.shape[1] // HEAD_DIM
    group_size = query_rows.shape[1] // key_rows.shape[1]
    sequences = row_count // SEQ
    grouped_query = query_rows.reshape(sequences, SEQ, key_heads, group_size, HEAD_DIM)
    grouped_key = key_rows.reshape(sequences, SEQ, key_heads, HEAD_DIM)
    scores = jnp.einsum(
        "bqkgd,bskd->bkgqs", grouped_query, grouped_key, preferred_element_type=jnp.float32
    ) * HEAD_DIM ** (-0.5)
    causal_mask = lax.broadcasted_iota(jnp.int32, (SEQ, SEQ), 0) >= lax.broadcasted_iota(
        jnp.int32, (SEQ, SEQ), 1
    )
    scores = jnp.where(causal_mask, scores, -1e30)
    highest = jnp.max(scores, axis=4, keepdims=True)
    raised = jnp.exp(scores - highest)
    return (raised / jnp.sum(raised, axis=4, keepdims=True)).astype(jnp.bfloat16)


def mix_values(attention, value_rows):
    sequences = attention.shape[0]
    key_heads = attention.shape[1]
    group_size = attention.shape[2]
    grouped_value = value_rows.reshape(sequences, SEQ, key_heads, HEAD_DIM)
    combined = jnp.einsum(
        "bkgqs,bskd->bqkgd", attention, grouped_value, preferred_element_type=jnp.float32
    )
    return combined.reshape(sequences * SEQ, key_heads * group_size * HEAD_DIM)


def spread_back(attention, upstream):
    sequences = attention.shape[0]
    key_heads = attention.shape[1]
    group_size = attention.shape[2]
    grouped_upstream = upstream.reshape(sequences, SEQ, key_heads, group_size, HEAD_DIM)
    spread = jnp.einsum(
        "bkgqs,bqkgd->bskd", attention, grouped_upstream, preferred_element_type=jnp.float32
    )
    return spread.reshape(sequences * SEQ, key_heads * HEAD_DIM)


def body(hidden, norm_gain, query_weight, key_weight, value_weight, output_weight, probe_seed):
    seed_value = probe_seed[0]
    normed = normalize(hidden, norm_gain)
    model_width = normed.shape[1]
    query_width = query_weight.shape[1]
    key_width = key_weight.shape[1]
    contract_rows = (((0,), (0,)), ((), ()))
    wide_tables, out_tables = gather_all(query_weight, key_weight, value_weight, output_weight)
    f32 = dict(preferred_element_type=jnp.float32)
    query_raw = jnp.concatenate([jnp.dot(normed, wide_tables[h, :, :512], **f32) for h in range(4)], 1)
    key_raw = jnp.concatenate([jnp.dot(normed, wide_tables[h, :, 512:640], **f32) for h in range(4)], 1)
    value_raw = jnp.concatenate([jnp.dot(normed, wide_tables[h, :, 640:], **f32) for h in range(4)], 1)
    query_rows = rotate(query_raw, query_width // HEAD_DIM)
    key_rows = rotate(key_raw, key_width // HEAD_DIM)
    value_rows = value_raw.astype(jnp.bfloat16)
    attention = attend(query_rows, key_rows)
    context = mix_values(attention, value_rows).astype(jnp.bfloat16)
    signs_value = sign_table(seed_value, 0, model_width, key_width)
    signs_out = sign_table(seed_value, 1, query_width, model_width)
    tangent_value = (jnp.dot(normed, signs_value, **f32) * model_width ** (-0.5)).astype(jnp.bfloat16)
    tangent_context = mix_values(attention, tangent_value).astype(jnp.bfloat16)
    probe_part = jnp.dot(context, signs_out, **f32) * query_width ** (-0.5)
    forward_part = jnp.concatenate([jnp.dot(tangent_context, out_tables[j], **f32) for j in range(4)], 1)
    cotangent = (forward_part + probe_part).astype(jnp.bfloat16)
    back_context = sum(
        lax.dot_general(
            cotangent[:, 512 * j : 512 * j + 512], out_tables[j], (((1,), (1,)), ((), ())), **f32
        )
        for j in range(4)
    )
    back_value = spread_back(attention, back_context.astype(jnp.bfloat16)).astype(jnp.bfloat16)
    term_value = jnp.stack(
        [
            lax.dot_general(normed, back_value[:, 128 * p : 128 * p + 128], contract_rows, **f32).astype(
                jnp.bfloat16
            )
            for p in range(4)
        ]
    )
    term_out = jnp.stack(
        [
            lax.dot_general(context, cotangent[:, 512 * p : 512 * p + 512], contract_rows, **f32).astype(
                jnp.bfloat16
            )
            for p in range(4)
        ]
    )
    return tuple(reduce_all(term_value, term_out))


def solution(mesh):
    return jax.shard_map(
        body,
        mesh=mesh,
        in_specs=(
            P(("probe", "fsdp"), None),
            P(),
            P("fsdp", None),
            P("fsdp", None),
            P("fsdp", None),
            P("fsdp", None),
            P("probe"),
        ),
        out_specs=(P("fsdp", "probe"), P("fsdp", "probe")),
        check_vma=False,
    )
```

```python
import jax
import jax.numpy as jnp
import numpy as np
from jax import lax
from jax.experimental import pallas as pl
from jax.experimental.pallas import tpu as pltpu
from jax.sharding import PartitionSpec as P

MESH = pl.DeviceIdType.MESH
HEAD_DIM = 128
SEQ = 256
norm_eps = 1e-05
rope_base = 500000.0


class Place:
    def __init__(self):
        p = lax.axis_index("probe")
        f = lax.axis_index("fsdp")
        self.p, self.f = p, f
        self.x = lax.rem(f, 4)
        self.zl = lax.rem(lax.div(f, 4), 2)
        self.y = lax.div(f, 8)
        self.zh = lax.div(p, 2)
        self.c = lax.rem(p, 2)
        self.z = self.zh * 2 + self.zl

    def move(self, axis, step):
        x, y, z = self.x, self.y, self.z
        if axis == "x":
            x = lax.rem(x + step + 4, 4)
        elif axis == "y":
            y = lax.rem(y + step + 4, 4)
        else:
            z = lax.rem(z + step + 4, 4)
        return (lax.div(z, 2) * 2 + self.c, y * 8 + lax.rem(z, 2) * 4 + x)

    def partner(self):
        return (self.zh * 2 + 1 - self.c, self.f)

    def neighbours(self):
        return [self.move(a, s) for a in ("x", "y", "z") for s in (1, -1)] + [self.partner()]


def meet(place):
    barrier = pltpu.get_barrier_semaphore()
    peers = place.neighbours()
    for peer in peers:
        pl.semaphore_signal(barrier, inc=1, device_id=peer, device_id_type=MESH)
    pl.semaphore_wait(barrier, len(peers))


class Copies:
    def __init__(self, send_sems, recv_sems):
        self.send_sems, self.recv_sems = send_sems, recv_sems
        self.used = 0
        self.started = []

    def slot(self):
        self.used += 1
        return self.used - 1

    def send(self, slot, ref, peer, dst=None):
        copy = pltpu.make_async_remote_copy(
            src_ref=ref,
            dst_ref=ref if dst is None else dst,
            send_sem=self.send_sems.at[slot],
            recv_sem=self.recv_sems.at[slot],
            device_id=peer,
            device_id_type=MESH,
        )
        copy.start()
        self.started.append(copy)

    def wait_recv(self, slot, ref, peer):
        pltpu.make_async_remote_copy(
            src_ref=ref,
            dst_ref=ref,
            send_sem=self.send_sems.at[slot],
            recv_sem=self.recv_sems.at[slot],
            device_id=peer,
            device_id_type=MESH,
        ).wait_recv()

    def finish(self):
        for copy in self.started:
            copy.wait_send()


def gather_steps(buf, order, place, copies):
    def region(have, where, core, halves):
        def pick(axis, extent):
            return pl.ds(0, extent) if axis in have else pl.ds(where[axis], 1)

        return buf.at[pick("y", 4), pick("z", 2), pick("x", 4), core, halves]

    here = {"x": place.x, "y": place.y, "z": place.zl}
    core, other = place.c, 1 - place.c
    partner = place.partner()
    from_partner = []

    def share(have, where):
        slot = copies.slot()
        copies.send(slot, region(have, where, core, pl.ds(0, 2)), partner)
        from_partner.append((slot, region(have, where, other, pl.ds(0, 2))))

    have = ()
    for phase, axis in enumerate(order):
        last = phase == 2
        if last:
            share(have, here)
        if axis == "z":
            slots = (copies.slot(), copies.slot())
            for half, step in ((0, 1), (1, -1)):
                copies.send(
                    slots[half], region(have, here, core, pl.ds(half, 1)), place.move("z", step)
                )
            there = dict(here, z=1 - place.zl)
            for half, step in ((0, -1), (1, 1)):
                yield
                copies.wait_recv(
                    slots[half], region(have, there, core, pl.ds(half, 1)), place.move("z", step)
                )
            if last:
                share(have, there)
        else:
            at = {s: dict(here, **{axis: lax.rem(here[axis] + s + 4, 4)}) for s in (-1, 1, 2)}
            up, down, up2, down2 = (copies.slot() for _ in range(4))
            ahead, behind = place.move(axis, 1), place.move(axis, -1)
            copies.send(up, region(have, here, core, pl.ds(0, 2)), ahead)
            copies.send(down, region(have, here, core, pl.ds(0, 2)), behind)
            yield
            copies.wait_recv(up, region(have, at[-1], core, pl.ds(0, 2)), behind)
            copies.send(up2, region(have, at[-1], core, pl.ds(0, 1)), ahead)
            if last:
                share(have, at[-1])
            yield
            copies.wait_recv(down, region(have, at[1], core, pl.ds(0, 2)), ahead)
            copies.send(down2, region(have, at[1], core, pl.ds(1, 1)), behind)
            if last:
                share(have, at[1])
            yield
            copies.wait_recv(up2, region(have, at[2], core, pl.ds(0, 1)), behind)
            yield
            copies.wait_recv(down2, region(have, at[2], core, pl.ds(1, 1)), ahead)
            if last:
                share(have, at[2])
        have = have + (axis,)
    for slot, ref in from_partner:
        yield
        copies.wait_recv(slot, ref, partner)


def in_turn(walks):
    walks = list(walks)
    while walks:
        left = []
        for walk in walks:
            try:
                next(walk)
                left.append(walk)
            except StopIteration:
                pass
        walks = left


def wrap32(value):
    value &= 0xFFFFFFFF
    return value - (1 << 32) if value >= 1 << 31 else value


MIX = 747796405


def fill_signs(dst, seed, code, table_columns, first_row, row_total, first_column):
    width = dst.shape[1]
    step = 32
    lanes = lax.broadcasted_iota(jnp.int32, (step, width), 1)
    tile = (lax.broadcasted_iota(jnp.int32, (step, width), 0) * table_columns + lanes) * MIX
    base = seed * 1664525 + wrap32(code * 374761393 + first_column * MIX)

    def one(i, carry):
        row = first_row + i * step
        hashed = tile + (base + row * wrap32(table_columns * MIX))
        hashed = hashed ^ lax.shift_right_logical(hashed, jnp.int32(15))
        hashed = hashed * 668265261
        hashed = hashed ^ lax.shift_right_logical(hashed, jnp.int32(13))
        hashed = hashed * 1274126177
        hashed = hashed ^ lax.shift_right_logical(hashed, jnp.int32(16))
        signs = jnp.where((hashed & 1) == 1, jnp.float32(1.0), jnp.float32(-1.0))
        dst[pl.ds(pl.multiple_of(row, step), step), :] = signs.astype(jnp.bfloat16)
        return carry

    lax.fori_loop(0, row_total // step, one, 0)


def dot(a, b):
    return jnp.dot(a, b, preferred_element_type=jnp.float32)


def dot_t(a, b):
    return lax.dot_general(a, b, (((1,), (1,)), ((), ())), preferred_element_type=jnp.float32)


def front_kernel(
    seed_ref, hidden, gain, turns, wq, wk, wv, wo,
    normed_t, context_t, cotangent_u, back_value,
    qkv, out, normed, signs, tangent, query, key, value, weights, context, tangent_context, part,
    cotangent, send_sems, recv_sems, load_sems,
):
    place = Place()
    bf16 = jnp.bfloat16
    loads = []

    def load(src, dst):
        copy = pltpu.make_async_copy(src, dst, load_sems.at[len(loads)])
        copy.start()
        loads.append(copy)

    def own(buf, columns):
        return buf.at[place.y, place.zl, place.x, place.c, :, :, columns]

    def rows(w, columns):
        return w.at[place.c, :, :, columns]

    for h in range(4):
        load(rows(wq, pl.ds(h * 512, 512)), own(qkv.at[h], pl.ds(0, 512)))
        load(rows(wk, pl.ds(h * 128, 128)), own(qkv.at[h], pl.ds(512, 128)))
        load(rows(wv, pl.ds(h * 128, 128)), own(qkv.at[h], pl.ds(640, 128)))
    for j in range(4):
        load(rows(wo, pl.ds(j * 512, 512)), own(out.at[j], pl.ds(0, 512)))
    meet(place)
    for copy in loads:
        copy.wait()
    copies = Copies(send_sems, recv_sems)
    seed = seed_ref[0]

    def norm(i):
        at = pl.ds(128 * i, 128)
        x = hidden[at, :].astype(jnp.float32)
        inverse = lax.rsqrt(jnp.mean(x * x, axis=1, keepdims=True) + norm_eps)
        n = (x * inverse * gain[...].astype(jnp.float32)).astype(bf16)
        normed[at, :] = n
        normed_t[:, at] = n.T

    def tangents(i):
        table = signs.at[0, :, pl.ds(256 * i, 256)]
        fill_signs(table, seed, 0, 512, 0, 2048, 256 * i)
        tangent[:, pl.ds(256 * i, 256)] = (dot(normed[...], table[...]) * 2048**-0.5).astype(bf16)

    def sign_part(i):
        fill_signs(signs.at[i // 2], seed, 1, 2048, 1024 * (i % 2), 1024, 512 * (i // 2))

    def project(h):
        cosine = jnp.concatenate([turns[0], turns[0]], 0)
        sine = jnp.concatenate([turns[1], turns[1]], 0)

        def rope(x):
            return (x * cosine + pltpu.roll(x, 64, 1) * sine).astype(bf16)

        for block in range(3):
            table = qkv[h, :, :, :, :, :, :, pl.ds(256 * block, 256)].reshape(2048, 256)
            raw = dot(normed[...], table)
            left, right = raw[:, :128], raw[:, 128:]
            if block < 2:
                query[2 * block] = rope(left)
                query[2 * block + 1] = rope(right)
            else:
                key[...] = rope(left)
                value[:, pl.ds(0, 128)] = right.astype(bf16)
                value[:, pl.ds(128, 128)] = tangent[:, pl.ds(128 * h, 128)]

    def attend(h, g):
        causal = lax.broadcasted_iota(jnp.int32, (SEQ, SEQ), 0) >= lax.broadcasted_iota(
            jnp.int32, (SEQ, SEQ), 1
        )
        head = pl.ds(128 * (4 * h + g), 128)
        for s in range(2):
            at = pl.ds(SEQ * s, SEQ)
            scores = dot_t(query[g, at, :], key[at, :]) * HEAD_DIM**-0.5
            scores = jnp.where(causal, scores, -1e30)
            raised = jnp.exp(scores - jnp.max(scores, axis=1, keepdims=True))
            chances = (raised * (1.0 / jnp.sum(raised, axis=1, keepdims=True))).astype(bf16)
            weights[h, s, g] = chances
            mixed = dot(chances, value[at, :]).astype(bf16)
            context[at, head] = mixed[:, :128]
            tangent_context[at, head] = mixed[:, 128:]
            context_t[head, at] = mixed[:, :128].T

    def probe(j):
        for block in range(2):
            at = pl.ds(256 * block, 256)
            part[j, :, at] = dot(context[...], signs[j, :, at]) * 2048**-0.5

    def forward(j):
        for block in range(2):
            at = pl.ds(256 * block, 256)
            table = out[j, :, :, :, :, :, :, at].reshape(2048, 256)
            total = (dot(tangent_context[...], table) + part[j, :, at]).astype(bf16)
            cotangent[:, pl.ds(512 * j + 256 * block, 256)] = total
            for side in range(2):
                cotangent_u[2 * block + side, :, pl.ds(128 * j, 128)] = total[
                    :, 128 * side : 128 * side + 128
                ]

    def back(h):
        table = jnp.concatenate([out[j, h].reshape(512, 512) for j in range(4)], 1)
        for s in range(2):
            at = pl.ds(SEQ * s, SEQ)
            turned = dot_t(table, cotangent[at, :]).astype(bf16)
            wide_row = jnp.concatenate([turned[128 * g : 128 * g + 128] for g in range(4)], 1)
            spread = dot(wide_row, weights[h, s].reshape(1024, SEQ)).astype(bf16)
            back_value[at, pl.ds(128 * h, 128)] = spread.T

    walks = [gather_steps(qkv.at[h], GATHER_ORDERS[h], place, copies) for h in range(4)]
    walks += [gather_steps(out.at[j], GATHER_ORDERS[j], place, copies) for j in range(4)]
    tasks = dict(n=norm, t=tangents, s=sign_part, q=project, a=attend, p=probe, f=forward, b=back)
    for what, *where in SCHEDULE:
        if what == "w":
            next(walks[where[0]], None)
        else:
            tasks[what](*where)
    copies.finish()


def front(seed, hidden, gain, turns, wq, wk, wv, wo):
    bf16 = jnp.bfloat16
    halves = [w.reshape(2, 2, 16, w.shape[1]) for w in (wq, wk, wv, wo)]
    copies = 120
    anywhere = pl.BlockSpec(memory_space=pl.ANY)
    vmem = pl.BlockSpec(memory_space=pltpu.VMEM)
    shapes = [(2048, 512), (2048, 512), (4, 512, 512), (512, 512)]
    scratch = [
        (4, 4, 2, 4, 2, 2, 16, 768),
        (4, 4, 2, 4, 2, 2, 16, 512),
        (512, 2048),
        (4, 2048, 512),
        (512, 512),
        (4, 512, 128),
        (512, 128),
        (512, 256),
        (4, 2, 4, SEQ, SEQ),
        (512, 2048),
        (512, 2048),
    ]
    return pl.pallas_call(
        front_kernel,
        out_shape=[jax.ShapeDtypeStruct(s, bf16) for s in shapes],
        in_specs=[pl.BlockSpec(memory_space=pltpu.SMEM)] + [vmem] * 3 + [anywhere] * 4,
        out_specs=[vmem] * 4,
        scratch_shapes=[pltpu.VMEM(s, bf16) for s in scratch]
        + [
            pltpu.VMEM((4, 512, 512), jnp.float32),
            pltpu.VMEM((512, 2048), bf16),
            pltpu.SemaphoreType.DMA((copies,)),
            pltpu.SemaphoreType.DMA((copies,)),
            pltpu.SemaphoreType.DMA((16,)),
        ],
        compiler_params=pltpu.CompilerParams(
            collective_id=0, has_side_effects=True, vmem_limit_bytes=63 * 1024 * 1024
        ),
    )(seed, hidden, gain.reshape(1, -1), turns, *halves)


def turn_tables():
    exponent = np.arange(64, dtype=np.float64) * (-2.0 / HEAD_DIM)
    angles = np.arange(SEQ, dtype=np.float64)[:, None] * np.power(rope_base, exponent)[None, :]
    cosine, sine = np.cos(angles), np.sin(angles)
    return np.stack(
        [np.concatenate([cosine, cosine], 1), np.concatenate([-sine, sine], 1)]
    ).astype(np.float32)


GATHER_ORDERS = (('x', 'y', 'z'), ('y', 'x', 'z'), ('z', 'x', 'y'), ('z', 'y', 'x'))
SCHEDULE = (
    ('w', 0),
    ('w', 1),
    ('w', 2),
    ('w', 3),
    ('w', 4),
    ('n', 0),
    ('n', 1),
    ('n', 2),
    ('n', 3),
    ('w', 2),
    ('w', 2),
    ('w', 0),
    ('w', 0),
    ('w', 1),
    ('w', 1),
    ('w', 3),
    ('w', 3),
    ('t', 0),
    ('w', 4),
    ('w', 4),
    ('w', 1),
    ('w', 1),
    ('t', 1),
    ('w', 0),
    ('w', 0),
    ('w', 2),
    ('w', 2),
    ('w', 3),
    ('w', 3),
    ('w', 4),
    ('w', 4),
    ('s', 0),
    ('s', 1),
    ('s', 2),
    ('w', 1),
    ('w', 1),
    ('s', 3),
    ('w', 2),
    ('w', 2),
    ('w', 0),
    ('w', 0),
    ('s', 4),
    ('w', 3),
    ('w', 3),
    ('s', 5),
    ('w', 1),
    ('w', 1),
    ('s', 6),
    ('w', 4),
    ('w', 4),
    ('s', 7),
    ('w', 3),
    ('w', 3),
    ('w', 2),
    ('w', 2),
    ('w', 1),
    ('w', 1),
    ('w', 1),
    ('w', 0),
    ('w', 0),
    ('w', 4),
    ('w', 4),
    ('w', 3),
    ('w', 3),
    ('w', 3),
    ('w', 3),
    ('w', 3),
    ('w', 2),
    ('w', 2),
    ('w', 2),
    ('w', 2),
    ('w', 2),
    ('w', 1),
    ('w', 5),
    ('q', 1),
    ('a', 1, 0),
    ('w', 5),
    ('w', 5),
    ('a', 1, 1),
    ('w', 0),
    ('w', 0),
    ('w', 0),
    ('a', 1, 2),
    ('w', 3),
    ('w', 5),
    ('w', 5),
    ('w', 6),
    ('a', 1, 3),
    ('w', 2),
    ('w', 7),
    ('q', 2),
    ('w', 0),
    ('w', 4),
    ('w', 4),
    ('w', 4),
    ('w', 6),
    ('w', 6),
    ('a', 2, 0),
    ('w', 5),
    ('w', 5),
    ('w', 7),
    ('w', 7),
    ('a', 2, 1),
    ('a', 2, 2),
    ('w', 4),
    ('w', 6),
    ('w', 6),
    ('a', 2, 3),
    ('w', 5),
    ('w', 5),
    ('w', 7),
    ('w', 7),
    ('q', 0),
    ('w', 6),
    ('w', 6),
    ('a', 0, 0),
    ('w', 7),
    ('w', 7),
    ('a', 0, 1),
    ('a', 0, 2),
    ('a', 0, 3),
    ('q', 3),
    ('w', 5),
    ('w', 5),
    ('w', 5),
    ('a', 3, 0),
    ('w', 6),
    ('w', 6),
    ('a', 3, 1),
    ('w', 7),
    ('w', 7),
    ('a', 3, 2),
    ('w', 5),
    ('a', 3, 3),
    ('p', 0),
    ('w', 6),
    ('w', 6),
    ('w', 6),
    ('w', 6),
    ('w', 6),
    ('p', 1),
    ('w', 7),
    ('w', 7),
    ('w', 7),
    ('w', 7),
    ('w', 7),
    ('p', 2),
    ('p', 3),
    ('w', 6),
    ('f', 0),
    ('w', 7),
    ('f', 1),
    ('f', 2),
    ('f', 3),
    ('b', 0),
    ('b', 1),
    ('b', 2),
    ('b', 3),
)


REDUCE_ORDERS = (("x", "y", "z"), ("y", "z", "x"), ("x", "z", "y"), ("y", "x", "z"), ("z", "x", "y"))


def wide(value):
    return value.astype(jnp.float32)


def reduce_steps(fill, order, mine, given, theirs, landing, result, place, copies):
    here = {"x": place.x, "y": place.y, "z": place.z}

    def region(done, where, half):
        at = dict(where)

        def pick(axis, extent):
            return pl.ds(at[axis], 1) if axis in done else pl.ds(0, extent)

        if "z" in done:
            zh, zl = pl.ds(lax.div(at["z"], 2), 1), pl.ds(lax.rem(at["z"], 2), 1)
        else:
            zh, zl = pl.ds(0, 2), pl.ds(0, 2)
        return mine.at[zh, pick("y", 4), zl, pick("x", 4), half]

    fill()
    partner_slot = copies.slot()
    copies.send(partner_slot, given, place.partner(), dst=theirs)
    yield
    copies.wait_recv(partner_slot, theirs, place.partner())

    def add_partner(i, carry):
        zh, y = lax.div(i, 4), lax.rem(i, 4)
        mine[zh, y] = (wide(mine[zh, y]) + wide(theirs[zh, y])).astype(jnp.bfloat16)
        return carry

    lax.fori_loop(0, 8, add_partner, 0)
    done = ()
    for stage, axis in enumerate(order):
        land = landing[stage]
        done = done + (axis,)
        at = {s: dict(here, **{axis: lax.rem(here[axis] + s + 4, 4)}) for s in (-1, 0, 1, 2)}
        ahead, behind = place.move(axis, 1), place.move(axis, -1)
        slots = [copies.slot() for _ in range(6)]

        def send(slot, step, half, peer):
            copies.send(slots[slot], region(done, at[step], half), peer, dst=land.at[slot])

        def wait(slot, peer):
            copies.wait_recv(slots[slot], land.at[slot], peer)

        send(0, 2, 0, ahead)
        send(1, 2, 1, behind)
        send(3, 1, 1, ahead)
        send(4, -1, 0, behind)
        yield
        for slot, step, half, source, peer, onward in (
            (0, 1, 0, behind, ahead, 2),
            (1, -1, 1, ahead, behind, 5),
        ):
            wait(slot, source)
            part = region(done, at[step], half)
            part[...] = (wide(part[...]) + wide(land[slot])).astype(jnp.bfloat16)
            send(onward, step, half, peer)
        yield
        for slot, source in ((3, behind), (4, ahead), (2, behind), (5, ahead)):
            wait(slot, source)
        for half in (0, 1):
            part = region(done, at[0], half)
            total = wide(part[...]) + wide(land[2 + half]) + wide(land[4 + half])
            if stage == 2:
                result[pl.ds(32 * half, 32), :] = total.reshape(32, 128)
            else:
                part[...] = total.astype(jnp.bfloat16)


def stage_shape(order, stage):
    done = order[: stage + 1]
    z = 1 if "z" in done else 2
    return (6, z, 1 if "y" in done else 4, z, 1 if "x" in done else 4, 32, 128)


def reduce_kernel(
    normed_t, context_t, cotangent_u, back_value, value_ref, out_ref, terms, theirs, *rest
):
    landing, (send_sems, recv_sems) = rest[:15], rest[15:]
    place = Place()
    copies = Copies(send_sems, recv_sems)
    meet(place)

    def filler(unit):
        def fill():
            left = normed_t if unit == 4 else context_t
            right = back_value if unit == 4 else cotangent_u.at[unit]

            def one(y, carry):
                rows = left[pl.ds(pl.multiple_of(512 * y, 512), 512), :]
                for zh in range(2):
                    both = dot(rows, right[:, pl.ds(256 * zh, 256)]).astype(jnp.bfloat16)
                    for core in range(2):
                        terms[unit, zh, core, y] = both[:, 128 * core : 128 * core + 128].reshape(
                            2, 4, 2, 32, 128
                        )
                return carry

            lax.fori_loop(0, 4, one, 0)

        return fill

    walks = [
        reduce_steps(
            filler(unit),
            REDUCE_ORDERS[unit],
            terms.at[unit, :, place.c],
            terms.at[unit, :, 1 - place.c],
            theirs.at[unit],
            landing[3 * unit : 3 * unit + 3],
            value_ref if unit == 4 else out_ref.at[:, pl.ds(128 * unit, 128)],
            place,
            copies,
        )
        for unit in range(5)
    ]
    for unit in REDUCE_START:
        next(walks[unit], None)
    in_turn(walks)
    copies.finish()


REDUCE_START = (0, 1, 0, 2, 1, 3, 2, 4, 0, 3, 4)


def reduce_all(normed_t, context_t, cotangent_u, back_value):
    table = (2, 4, 2, 4, 2, 32, 128)
    copies = 5 * 19
    vmem = pl.BlockSpec(memory_space=pltpu.VMEM)
    return pl.pallas_call(
        reduce_kernel,
        out_shape=[
            jax.ShapeDtypeStruct((64, 128), jnp.float32),
            jax.ShapeDtypeStruct((64, 512), jnp.float32),
        ],
        in_specs=[vmem] * 4,
        out_specs=[vmem] * 2,
        scratch_shapes=[
            pltpu.VMEM((5, 2, 2) + table[1:], jnp.bfloat16),
            pltpu.VMEM((5,) + table, jnp.bfloat16),
        ]
        + [
            pltpu.VMEM(stage_shape(REDUCE_ORDERS[unit], stage), jnp.bfloat16)
            for unit in range(5)
            for stage in range(3)
        ]
        + [pltpu.SemaphoreType.DMA((copies,)), pltpu.SemaphoreType.DMA((copies,))],
        compiler_params=pltpu.CompilerParams(
            collective_id=1, has_side_effects=True, vmem_limit_bytes=48 * 1024 * 1024
        ),
    )(normed_t, context_t, cotangent_u, back_value)


def body(hidden, norm_gain, query_weight, key_weight, value_weight, output_weight, probe_seed):
    parts = front(
        probe_seed,
        hidden,
        norm_gain,
        jnp.asarray(turn_tables()),
        query_weight,
        key_weight,
        value_weight,
        output_weight,
    )
    return tuple(reduce_all(*parts))


def solution(mesh):
    return jax.shard_map(
        body,
        mesh=mesh,
        in_specs=(
            P(("probe", "fsdp"), None),
            P(),
            P("fsdp", None),
            P("fsdp", None),
            P("fsdp", None),
            P("fsdp", None),
            P("probe"),
        ),
        out_specs=(P("fsdp", "probe"), P("fsdp", "probe")),
        check_vma=False,
    )
```

```python
import jax
import jax.numpy as jnp
import numpy as np
from jax import lax
from jax.experimental import pallas as pl
from jax.experimental.pallas import tpu as pltpu
from jax.sharding import PartitionSpec as P

MESH = pl.DeviceIdType.MESH
HEAD_DIM = 128
SEQ = 256
norm_eps = 1e-05
rope_base = 500000.0


class Place:
    def __init__(self):
        p = lax.axis_index("probe")
        f = lax.axis_index("fsdp")
        self.p, self.f = p, f
        self.x = lax.rem(f, 4)
        self.zl = lax.rem(lax.div(f, 4), 2)
        self.y = lax.div(f, 8)
        self.zh = lax.div(p, 2)
        self.c = lax.rem(p, 2)
        self.z = self.zh * 2 + self.zl

    def move(self, axis, step):
        x, y, z = self.x, self.y, self.z
        if axis == "x":
            x = lax.rem(x + step + 4, 4)
        elif axis == "y":
            y = lax.rem(y + step + 4, 4)
        else:
            z = lax.rem(z + step + 4, 4)
        return (lax.div(z, 2) * 2 + self.c, y * 8 + lax.rem(z, 2) * 4 + x)

    def partner(self):
        return (self.zh * 2 + 1 - self.c, self.f)

    def neighbours(self):
        return [self.move(a, s) for a in ("x", "y", "z") for s in (1, -1)] + [self.partner()]


def meet(place):
    barrier = pltpu.get_barrier_semaphore()
    peers = place.neighbours()
    for peer in peers:
        pl.semaphore_signal(barrier, inc=1, device_id=peer, device_id_type=MESH)
    pl.semaphore_wait(barrier, len(peers))


class Copies:
    def __init__(self, send_sems, recv_sems):
        self.send_sems, self.recv_sems = send_sems, recv_sems
        self.used = 0
        self.early = False
        self.started = []

    def slot(self):
        self.used += 1
        return self.used - 1

    def send(self, slot, ref, peer, dst=None):
        copy = pltpu.make_async_remote_copy(
            src_ref=ref,
            dst_ref=ref if dst is None else dst,
            send_sem=self.send_sems.at[slot],
            recv_sem=self.recv_sems.at[slot],
            device_id=peer,
            device_id_type=MESH,
        )
        copy.start()
        self.started.append((self.early, copy))

    def wait_recv(self, slot, ref, peer):
        pltpu.make_async_remote_copy(
            src_ref=ref,
            dst_ref=ref,
            send_sem=self.send_sems.at[slot],
            recv_sem=self.recv_sems.at[slot],
            device_id=peer,
            device_id_type=MESH,
        ).wait_recv()

    def finish(self, early_only=False):
        for early, copy in self.started:
            if early or not early_only:
                copy.wait_send()
        self.started = [s for s in self.started if early_only and not s[0]]


def gather_steps(buf, order, place, copies):
    def region(have, where, core, halves):
        def pick(axis, extent):
            return pl.ds(0, extent) if axis in have else pl.ds(where[axis], 1)

        return buf.at[pick("y", 4), pick("z", 2), pick("x", 4), core, halves]

    here = {"x": place.x, "y": place.y, "z": place.zl}
    core, other = place.c, 1 - place.c
    partner = place.partner()
    from_partner = []

    def share(have, where):
        slot = copies.slot()
        copies.send(slot, region(have, where, core, pl.ds(0, 2)), partner)
        from_partner.append((slot, region(have, where, other, pl.ds(0, 2))))

    have = ()
    for phase, axis in enumerate(order):
        last = phase == 2
        if last:
            share(have, here)
        if axis == "z":
            slots = (copies.slot(), copies.slot())
            for half, step in ((0, 1), (1, -1)):
                copies.send(
                    slots[half], region(have, here, core, pl.ds(half, 1)), place.move("z", step)
                )
            there = dict(here, z=1 - place.zl)
            for half, step in ((0, -1), (1, 1)):
                yield
                copies.wait_recv(
                    slots[half], region(have, there, core, pl.ds(half, 1)), place.move("z", step)
                )
            if last:
                share(have, there)
        else:
            at = {s: dict(here, **{axis: lax.rem(here[axis] + s + 4, 4)}) for s in (-1, 1, 2)}
            up, down, up2, down2 = (copies.slot() for _ in range(4))
            ahead, behind = place.move(axis, 1), place.move(axis, -1)
            copies.send(up, region(have, here, core, pl.ds(0, 2)), ahead)
            copies.send(down, region(have, here, core, pl.ds(0, 2)), behind)
            yield
            copies.wait_recv(up, region(have, at[-1], core, pl.ds(0, 2)), behind)
            copies.send(up2, region(have, at[-1], core, pl.ds(0, 1)), ahead)
            if last:
                share(have, at[-1])
            yield
            copies.wait_recv(down, region(have, at[1], core, pl.ds(0, 2)), ahead)
            copies.send(down2, region(have, at[1], core, pl.ds(1, 1)), behind)
            if last:
                share(have, at[1])
            yield
            copies.wait_recv(up2, region(have, at[2], core, pl.ds(0, 1)), behind)
            yield
            copies.wait_recv(down2, region(have, at[2], core, pl.ds(1, 1)), ahead)
            if last:
                share(have, at[2])
        have = have + (axis,)
    for slot, ref in from_partner:
        yield
        copies.wait_recv(slot, ref, partner)


GATHER_ORDERS = (('y', 'x', 'z'), ('x', 'y', 'z'), ('z', 'y', 'x'), ('x', 'y', 'z'), ('x', 'y', 'z'), ('x', 'y', 'z'), ('y', 'x', 'z'), ('x', 'y', 'z'))
REDUCE_ORDERS = (('z', 'x', 'y'), ('x', 'z', 'y'), ('x', 'y', 'z'), ('x', 'y', 'z'), ('z', 'y', 'x'))
SCHEDULE = (
    ('w', 0),
    ('w', 1),
    ('w', 2),
    ('w', 3),
    ('w', 4),
    ('w', 5),
    ('n', 0),
    ('n', 1),
    ('n', 2),
    ('n', 3),
    ('w', 0),
    ('w', 0),
    ('w', 1),
    ('w', 1),
    ('w', 2),
    ('w', 2),
    ('t', 0),
    ('w', 0),
    ('w', 0),
    ('w', 1),
    ('w', 1),
    ('w', 3),
    ('w', 3),
    ('w', 4),
    ('w', 4),
    ('w', 5),
    ('w', 5),
    ('t', 1),
    ('w', 2),
    ('w', 2),
    ('s', 0),
    ('s', 1),
    ('s', 2),
    ('w', 0),
    ('w', 0),
    ('w', 1),
    ('w', 1),
    ('w', 2),
    ('w', 2),
    ('w', 3),
    ('w', 3),
    ('w', 4),
    ('w', 4),
    ('w', 5),
    ('w', 5),
    ('s', 3),
    ('s', 4),
    ('s', 5),
    ('w', 0),
    ('w', 0),
    ('w', 1),
    ('w', 1),
    ('s', 6),
    ('s', 7),
    ('w', 3),
    ('w', 3),
    ('w', 4),
    ('w', 4),
    ('w', 2),
    ('w', 2),
    ('w', 5),
    ('w', 5),
    ('w', 0),
    ('w', 0),
    ('w', 0),
    ('w', 3),
    ('w', 3),
    ('w', 4),
    ('w', 4),
    ('w', 2),
    ('w', 2),
    ('w', 2),
    ('w', 2),
    ('w', 2),
    ('w', 5),
    ('w', 5),
    ('w', 0),
    ('w', 6),
    ('q', 0),
    ('a', 0, 0),
    ('w', 6),
    ('w', 6),
    ('a', 0, 1),
    ('w', 1),
    ('w', 1),
    ('w', 1),
    ('a', 0, 2),
    ('w', 2),
    ('w', 6),
    ('w', 6),
    ('w', 7),
    ('a', 0, 3),
    ('q', 2),
    ('w', 1),
    ('a', 2, 0),
    ('a', 2, 1),
    ('w', 6),
    ('w', 6),
    ('w', 7),
    ('w', 7),
    ('w', 3),
    ('w', 3),
    ('w', 3),
    ('a', 2, 2),
    ('a', 2, 3),
    ('q', 1),
    ('w', 3),
    ('w', 6),
    ('w', 6),
    ('w', 7),
    ('w', 7),
    ('a', 1, 0),
    ('w', 4),
    ('w', 4),
    ('w', 4),
    ('a', 1, 1),
    ('a', 1, 2),
    ('a', 1, 3),
    ('w', 4),
    ('w', 7),
    ('w', 7),
    ('q', 3),
    ('w', 5),
    ('w', 5),
    ('w', 5),
    ('a', 3, 0),
    ('w', 7),
    ('w', 7),
    ('a', 3, 1),
    ('a', 3, 2),
    ('w', 5),
    ('a', 3, 3),
    ('w', 6),
    ('w', 6),
    ('w', 6),
    ('p', 0),
    ('f', 0),
    ('m', 0),
    ('w', 8),
    ('w', 6),
    ('p', 1),
    ('w', 7),
    ('w', 7),
    ('w', 7),
    ('f', 1),
    ('m', 1),
    ('w', 9),
    ('p', 2),
    ('w', 8),
    ('f', 2),
    ('w', 7),
    ('m', 2),
    ('w', 10),
    ('p', 3),
    ('w', 9),
    ('w', 8),
    ('w', 8),
    ('f', 3),
    ('m', 3),
    ('w', 11),
    ('w', 8),
    ('w', 8),
    ('w', 10),
    ('b', 0),
    ('w', 8),
    ('w', 8),
    ('w', 9),
    ('w', 9),
    ('w', 9),
    ('w', 9),
    ('b', 1),
    ('w', 11),
    ('w', 10),
    ('w', 10),
    ('b', 2),
    ('w', 10),
    ('w', 10),
    ('b', 3),
    ('w', 8),
    ('w', 8),
    ('w', 8),
    ('w', 8),
    ('m', 4),
    ('w', 12),
    ('w', 9),
    ('w', 9),
    ('w', 11),
    ('w', 11),
    ('w', 9),
    ('w', 9),
    ('w', 9),
    ('w', 9),
    ('w', 12),
    ('w', 9),
    ('w', 9),
    ('w', 11),
    ('w', 11),
    ('w', 10),
    ('w', 10),
    ('w', 8),
    ('w', 8),
    ('w', 9),
    ('w', 9),
    ('w', 9),
    ('w', 9),
    ('w', 12),
    ('w', 12),
    ('w', 10),
    ('w', 10),
    ('w', 11),
    ('w', 11),
    ('w', 8),
    ('w', 8),
    ('w', 8),
    ('w', 8),
    ('w', 9),
    ('w', 9),
    ('w', 10),
    ('w', 10),
    ('w', 12),
    ('w', 12),
    ('w', 10),
    ('w', 10),
    ('w', 11),
    ('w', 11),
    ('w', 11),
    ('w', 11),
    ('w', 8),
    ('w', 8),
    ('w', 12),
    ('w', 12),
    ('w', 10),
    ('w', 10),
    ('w', 10),
    ('w', 10),
    ('w', 11),
    ('w', 11),
    ('w', 10),
    ('w', 10),
    ('w', 12),
    ('w', 12),
    ('w', 12),
    ('w', 11),
    ('w', 11),
    ('w', 11),
    ('w', 11),
    ('w', 12),
    ('w', 12),
    ('w', 12),
    ('w', 11),
    ('w', 11),
    ('w', 12),
    ('w', 12),
    ('w', 12),
    ('w', 12),
    ('w', 12),
    ('w', 12),
)


def wide(value):
    return value.astype(jnp.float32)


def reduce_steps(order, table, first_lane, given, theirs, landing, result, place, copies):
    here = {"x": place.x, "y": place.y, "z": place.z}

    def region(done, where, half):
        def pick(axis, extent):
            return pl.ds(where[axis], 1) if axis in done else pl.ds(0, extent)

        zl, lanes = pl.ds(0, 2), pl.ds(first_lane, 256)
        if "z" in done:
            zl = pl.ds(lax.rem(where["z"], 2), 1)
            lanes = pl.ds(pl.multiple_of(first_lane + 128 * lax.div(where["z"], 2), 128), 128)
        return table.at[pick("y", 4), zl, pick("x", 4), half, :, :, lanes]

    partner_slot = copies.slot()
    copies.send(partner_slot, given, place.partner(), dst=theirs)
    yield
    copies.wait_recv(partner_slot, theirs, place.partner())

    def add_partner(y, carry):
        at = (y, slice(None), slice(None), slice(None), slice(None), slice(None), pl.ds(first_lane, 256))
        table[at] = (wide(table[at]) + wide(theirs[y])).astype(jnp.bfloat16)
        return carry

    lax.fori_loop(0, 4, add_partner, 0)
    done = ()
    for stage, axis in enumerate(order):
        land = landing[stage]
        done = done + (axis,)
        at = {s: dict(here, **{axis: lax.rem(here[axis] + s + 4, 4)}) for s in (-1, 0, 1, 2)}
        ahead, behind = place.move(axis, 1), place.move(axis, -1)
        slots = [copies.slot() for _ in range(6)]

        def send(slot, step, half, peer):
            copies.send(slots[slot], region(done, at[step], half), peer, dst=land.at[slot])

        def wait(slot, peer):
            copies.wait_recv(slots[slot], land.at[slot], peer)

        send(0, 2, 0, ahead)
        send(1, 2, 1, behind)
        send(3, 1, 1, ahead)
        send(4, -1, 0, behind)
        for slot, step, half, source, peer, onward in (
            (0, 1, 0, behind, ahead, 2),
            (1, -1, 1, ahead, behind, 5),
        ):
            yield
            wait(slot, source)
            part = region(done, at[step], half)
            part[...] = (wide(part[...]) + wide(land[slot])).astype(jnp.bfloat16)
            send(onward, step, half, peer)
        for slot, source in ((3, behind), (4, ahead), (2, behind), (5, ahead)):
            yield
            wait(slot, source)
        for half in (0, 1):
            part = region(done, at[0], half)
            total = wide(part[...]) + wide(land[2 + half]) + wide(land[4 + half])
            if stage == 2:
                result[pl.ds(32 * half, 32), :] = total.reshape(32, 128)
            else:
                part[...] = total.astype(jnp.bfloat16)


def stage_shape(order, stage):
    done = order[: stage + 1]
    x, y = (1 if axis in done else 4 for axis in "xy")
    zl, lanes = (1, 128) if "z" in done else (2, 256)
    return (6, y, zl, x, 2, 16, lanes)


def wrap32(value):
    value &= 0xFFFFFFFF
    return value - (1 << 32) if value >= 1 << 31 else value


MIX = 747796405


def fill_signs(dst, seed, code, table_columns, first_row, row_total, first_column, spread):
    width = dst.shape[1]
    step = 32
    lanes = lax.broadcasted_iota(jnp.int32, (step, width), 1)
    if spread:
        lanes = lanes + lax.div(lanes, 128) * 384
    tile = (lax.broadcasted_iota(jnp.int32, (step, width), 0) * table_columns + lanes) * MIX
    base = seed * 1664525 + wrap32(code * 374761393 + first_column * MIX)

    def one(i, carry):
        row = first_row + i * step
        hashed = tile + (base + row * wrap32(table_columns * MIX))
        hashed = hashed ^ lax.shift_right_logical(hashed, jnp.int32(15))
        hashed = hashed * 668265261
        hashed = hashed ^ lax.shift_right_logical(hashed, jnp.int32(13))
        hashed = hashed * 1274126177
        hashed = hashed ^ lax.shift_right_logical(hashed, jnp.int32(16))
        signs = jnp.where((hashed & 1) == 1, jnp.float32(1.0), jnp.float32(-1.0))
        dst[pl.ds(pl.multiple_of(row, step), step), :] = signs.astype(jnp.bfloat16)
        return carry

    lax.fori_loop(0, row_total // step, one, 0)


def dot(a, b):
    return jnp.dot(a, b, preferred_element_type=jnp.float32)


def dot_t(a, b):
    return lax.dot_general(a, b, (((1,), (1,)), ((), ())), preferred_element_type=jnp.float32)


def whole_kernel(
    seed_ref, gain, turns, hidden, wq, wk, wv, wo, value_ref, out_ref,
    qkv, out, normed, normed_t, signs, tangent, query, key, value, weights, context, context_t,
    tangent_context, part, cotangent, back_value, theirs, *rest,
):
    landing, (send_sems, recv_sems, load_sems) = rest[:15], rest[15:]
    place = Place()
    bf16 = jnp.bfloat16
    loads = []

    def load(src, dst):
        copy = pltpu.make_async_copy(src, dst, load_sems.at[len(loads)])
        copy.start()
        loads.append(copy)

    def own(buf, columns):
        return buf.at[place.y, place.zl, place.x, place.c, :, :, columns]

    def rows(w, columns):
        return w.at[place.c, :, :, columns]

    for h in range(4):
        load(rows(wq, pl.ds(h * 512, 512)), own(qkv.at[h], pl.ds(0, 512)))
        load(rows(wk, pl.ds(h * 128, 128)), own(qkv.at[h], pl.ds(512, 128)))
        load(rows(wv, pl.ds(h * 128, 128)), own(qkv.at[h], pl.ds(640, 128)))
    for j in range(4):
        for p in range(4):
            load(rows(wo, pl.ds(512 * p + 128 * j, 128)), own(out.at[j], pl.ds(128 * p, 128)))
    load(hidden, normed)
    meet(place)
    for copy in loads:
        copy.wait()
    copies = Copies(send_sems, recv_sems)
    seed = seed_ref[0]

    def norm(i):
        at = pl.ds(128 * i, 128)
        x = normed[at, :].astype(jnp.float32)
        inverse = lax.rsqrt(jnp.mean(x * x, axis=1, keepdims=True) + norm_eps)
        n = (x * inverse * gain[...][None, :].astype(jnp.float32)).astype(bf16)
        normed[at, :] = n
        normed_t[:, at] = n.T

    def tangents(i):
        table = signs.at[0, :, pl.ds(256 * i, 256)]
        fill_signs(table, seed, 0, 512, 0, 2048, 256 * i, False)
        tangent[:, pl.ds(256 * i, 256)] = (dot(normed[...], table[...]) * 2048**-0.5).astype(bf16)

    def sign_part(i):
        fill_signs(signs.at[i // 2], seed, 1, 2048, 1024 * (i % 2), 1024, 128 * (i // 2), True)

    def project(h):
        cosine = jnp.concatenate([turns[0], turns[0]], 0)
        sine = jnp.concatenate([turns[1], turns[1]], 0)

        def rope(x):
            return (x * cosine + pltpu.roll(x, 64, 1) * sine).astype(bf16)

        for block in range(3):
            table = qkv[h, :, :, :, :, :, :, pl.ds(256 * block, 256)].reshape(2048, 256)
            raw = dot(normed[...], table)
            left, right = raw[:, :128], raw[:, 128:]
            if block < 2:
                query[2 * block] = rope(left)
                query[2 * block + 1] = rope(right)
            else:
                key[...] = rope(left)
                value[:, pl.ds(0, 128)] = right.astype(bf16)
                value[:, pl.ds(128, 128)] = tangent[:, pl.ds(128 * h, 128)]

    def attend(h, g):
        causal = lax.broadcasted_iota(jnp.int32, (SEQ, SEQ), 0) >= lax.broadcasted_iota(
            jnp.int32, (SEQ, SEQ), 1
        )
        head = pl.ds(128 * (4 * h + g), 128)
        for s in range(2):
            at = pl.ds(SEQ * s, SEQ)
            scores = dot_t(query[g, at, :], key[at, :]) * HEAD_DIM**-0.5
            scores = jnp.where(causal, scores, -1e30)
            raised = jnp.exp(scores - jnp.max(scores, axis=1, keepdims=True))
            chances = (raised * (1.0 / jnp.sum(raised, axis=1, keepdims=True))).astype(bf16)
            weights[h, s, g] = chances
            mixed = dot(chances, value[at, :]).astype(bf16)
            context[at, head] = mixed[:, :128]
            tangent_context[at, head] = mixed[:, 128:]
            context_t[head, at] = mixed[:, :128].T

    def probe(j):
        for block in range(2):
            at = pl.ds(256 * block, 256)
            part[j, :, at] = (dot(context[...], signs[j, :, at]) * 2048**-0.5).astype(bf16)

    def forward(j):
        for block in range(2):
            at = pl.ds(256 * block, 256)
            table = out[j, :, :, :, :, :, :, at].reshape(2048, 256)
            total = (dot(tangent_context[...], table) + part[j, :, at].astype(jnp.float32)).astype(bf16)
            cotangent[:, pl.ds(512 * j + 256 * block, 256)] = total

    def back(h):
        table = jnp.concatenate([out[j, h].reshape(512, 512) for j in range(4)], 1)
        for s in range(2):
            at = pl.ds(SEQ * s, SEQ)
            turned = dot_t(table, cotangent[at, :]).astype(bf16)
            wide_row = jnp.concatenate([turned[128 * g : 128 * g + 128] for g in range(4)], 1)
            spread = dot(wide_row, weights[h, s].reshape(1024, SEQ)).astype(bf16)
            back_value[at, pl.ds(128 * h, 128)] = spread.T

    def own_term(unit, zh, core):
        side = lax.rem(place.c + core, 2)
        if unit == 4:
            return side, pl.ds(512 + 128 * zh, 128)
        return unit, pl.ds(pl.multiple_of(256 * side + 128 * zh, 128), 128)

    def terms(unit):
        if unit == TERM_FIRST:
            copies.finish(early_only=True)
        left = normed_t if unit == 4 else context_t

        def one(y, carry):
            rows = left[pl.ds(pl.multiple_of(512 * y, 512), 512), :]
            for zh in range(2):
                if unit == 4:
                    right = back_value[:, pl.ds(256 * zh, 256)]
                else:
                    right = cotangent[:, pl.ds(512 * unit + 256 * zh, 256)]
                both = dot(rows, right).astype(bf16)
                for core in range(2):
                    h, lanes = own_term(unit, zh, core)
                    qkv[h, y, :, :, :, :, :, lanes] = both[:, 128 * core : 128 * core + 128].reshape(
                        2, 4, 2, 2, 16, 128
                    )
            return carry

        lax.fori_loop(0, 4, one, 0)

    def reduce_walk(unit):
        mine = (0, 512) if unit == 4 else (unit, 0)
        given = qkv.at[1, :, :, :, :, :, :, pl.ds(512, 256)]
        if unit < 4:
            given = qkv.at[unit, :, :, :, :, :, :, pl.ds(256, 256)]
        return reduce_steps(
            REDUCE_ORDERS[unit],
            qkv.at[mine[0]],
            mine[1],
            given,
            theirs.at[unit],
            landing[3 * unit : 3 * unit + 3],
            value_ref if unit == 4 else out_ref.at[:, pl.ds(128 * unit, 128)],
            place,
            copies,
        )

    walks = [gather_steps(qkv.at[h], GATHER_ORDERS[h], place, copies) for h in range(4)]
    walks += [gather_steps(out.at[j], GATHER_ORDERS[4 + j], place, copies) for j in range(4)]
    walks += [reduce_walk(unit) for unit in range(5)]
    tasks = dict(
        n=norm, t=tangents, s=sign_part, q=project, a=attend, p=probe, f=forward, b=back, m=terms
    )
    for what, *where in SCHEDULE:
        if what == "w":
            copies.early = where[0] < 4
            next(walks[where[0]], None)
        else:
            tasks[what](*where)
    copies.finish()


TERM_FIRST = [where[0] for what, *where in SCHEDULE if what == "m"][0]


def whole(seed, hidden, gain, turns, wq, wk, wv, wo):
    bf16 = jnp.bfloat16
    halves = [w.reshape(2, 2, 16, w.shape[1]) for w in (wq, wk, wv, wo)]
    copies = 210
    anywhere = pl.BlockSpec(memory_space=pl.ANY)
    vmem = pl.BlockSpec(memory_space=pltpu.VMEM)
    scratch = [
        (4, 4, 2, 4, 2, 2, 16, 768),
        (4, 4, 2, 4, 2, 2, 16, 512),
        (512, 2048),
        (2048, 512),
        (4, 2048, 512),
        (512, 512),
        (4, 512, 128),
        (512, 128),
        (512, 256),
        (4, 2, 4, SEQ, SEQ),
        (512, 2048),
        (2048, 512),
        (512, 2048),
    ]
    landings = [stage_shape(REDUCE_ORDERS[u], stage) for u in range(5) for stage in range(3)]
    scratch += [(4, 512, 512), (512, 2048), (512, 512), (5, 4, 2, 4, 2, 2, 16, 256)] + landings
    return pl.pallas_call(
        whole_kernel,
        out_shape=[
            jax.ShapeDtypeStruct((64, 128), jnp.float32),
            jax.ShapeDtypeStruct((64, 512), jnp.float32),
        ],
        in_specs=[pl.BlockSpec(memory_space=pltpu.SMEM)] + [vmem] * 2 + [anywhere] * 5,
        out_specs=[vmem] * 2,
        scratch_shapes=[pltpu.VMEM(s, bf16) for s in scratch]
        + [
            pltpu.SemaphoreType.DMA((copies,)),
            pltpu.SemaphoreType.DMA((copies,)),
            pltpu.SemaphoreType.DMA((32,)),
        ],
        compiler_params=pltpu.CompilerParams(
            collective_id=0, has_side_effects=True, vmem_limit_bytes=67043328
        ),
    )(seed, gain, turns, hidden, *halves)


def turn_tables():
    exponent = np.arange(64, dtype=np.float64) * (-2.0 / HEAD_DIM)
    angles = np.arange(SEQ, dtype=np.float64)[:, None] * np.power(rope_base, exponent)[None, :]
    cosine, sine = np.cos(angles), np.sin(angles)
    return np.stack(
        [np.concatenate([cosine, cosine], 1), np.concatenate([-sine, sine], 1)]
    ).astype(np.float32)

def body(hidden, norm_gain, query_weight, key_weight, value_weight, output_weight, probe_seed):
    return tuple(
        whole(
            probe_seed,
            hidden,
            norm_gain,
            jnp.asarray(turn_tables()),
            query_weight,
            key_weight,
            value_weight,
            output_weight,
        )
    )


def solution(mesh):
    return jax.shard_map(
        body,
        mesh=mesh,
        in_specs=(
            P(("probe", "fsdp"), None),
            P(),
            P("fsdp", None),
            P("fsdp", None),
            P("fsdp", None),
            P("fsdp", None),
            P("probe"),
        ),
        out_specs=(P("fsdp", "probe"), P("fsdp", "probe")),
        check_vma=False,
    )
```

```python
import jax
import jax.numpy as jnp
import numpy as np
from jax import lax
from jax.experimental import pallas as pl
from jax.experimental.pallas import tpu as pltpu
from jax.sharding import PartitionSpec as P

MESH = pl.DeviceIdType.MESH
HEAD_DIM = 128
SEQ = 256
norm_eps = 1e-05
rope_base = 500000.0


class Place:
    def __init__(self):
        p = lax.axis_index("probe")
        f = lax.axis_index("fsdp")
        self.p, self.f = p, f
        self.x = lax.rem(f, 4)
        self.zl = lax.rem(lax.div(f, 4), 2)
        self.y = lax.div(f, 8)
        self.zh = lax.div(p, 2)
        self.c = lax.rem(p, 2)
        self.z = self.zh * 2 + self.zl

    def move(self, axis, step):
        x, y, z = self.x, self.y, self.z
        if axis == "x":
            x = lax.rem(x + step + 4, 4)
        elif axis == "y":
            y = lax.rem(y + step + 4, 4)
        else:
            z = lax.rem(z + step + 4, 4)
        return (lax.div(z, 2) * 2 + self.c, y * 8 + lax.rem(z, 2) * 4 + x)

    def partner(self):
        return (self.zh * 2 + 1 - self.c, self.f)

    def neighbours(self):
        return [self.move(a, s) for a in ("x", "y", "z") for s in (1, -1, 2)] + [self.partner()]


def greet(place):
    barrier = pltpu.get_barrier_semaphore()
    for peer in place.neighbours():
        pl.semaphore_signal(barrier, inc=1, device_id=peer, device_id_type=MESH)


def meet(place):
    pl.semaphore_wait(pltpu.get_barrier_semaphore(), len(place.neighbours()))


class Copies:
    def __init__(self, send_sems, recv_sems):
        self.send_sems, self.recv_sems = send_sems, recv_sems
        self.used = 0
        self.early = False
        self.started = []

    def slot(self):
        self.used += 1
        return self.used - 1

    def send(self, slot, ref, peer, dst=None):
        copy = pltpu.make_async_remote_copy(
            src_ref=ref,
            dst_ref=ref if dst is None else dst,
            send_sem=self.send_sems.at[slot],
            recv_sem=self.recv_sems.at[slot],
            device_id=peer,
            device_id_type=MESH,
        )
        copy.start()
        self.started.append((self.early, copy))

    def wait_recv(self, slot, ref, peer):
        pltpu.make_async_remote_copy(
            src_ref=ref,
            dst_ref=ref,
            send_sem=self.send_sems.at[slot],
            recv_sem=self.recv_sems.at[slot],
            device_id=peer,
            device_id_type=MESH,
        ).wait_recv()

    def finish(self, early_only=False):
        for early, copy in self.started:
            if early or not early_only:
                copy.wait_send()
        self.started = [s for s in self.started if early_only and not s[0]]


def gather_steps(buf, lanes, order, place, copies):
    def region(have, where, core, halves):
        def pick(axis, extent):
            return pl.ds(0, extent) if axis in have else pl.ds(where[axis], 1)

        return buf.at[pick("y", 4), pick("z", 2), pick("x", 4), core, halves, :, lanes]

    here = {"x": place.x, "y": place.y, "z": place.zl}
    core, other = place.c, 1 - place.c
    partner = place.partner()
    from_partner = []

    def share(have, where):
        slot = copies.slot()
        copies.send(slot, region(have, where, core, pl.ds(0, 2)), partner)
        from_partner.append((slot, region(have, where, other, pl.ds(0, 2))))

    have = ()
    for phase, axis in enumerate(order):
        last = phase == 2
        if last:
            share(have, here)
        if axis == "z":
            slots = (copies.slot(), copies.slot())
            for half, step in ((0, 1), (1, -1)):
                copies.send(
                    slots[half], region(have, here, core, pl.ds(half, 1)), place.move("z", step)
                )
            there = dict(here, z=1 - place.zl)
            for half, step in ((0, -1), (1, 1)):
                yield
                copies.wait_recv(
                    slots[half], region(have, there, core, pl.ds(half, 1)), place.move("z", step)
                )
            if last:
                share(have, there)
        elif phase == 0:
            slots = [copies.slot() for _ in range(3)]
            for slot, step in zip(slots, (-1, 1, 2)):
                copies.send(slot, region(have, here, core, pl.ds(0, 2)), place.move(axis, step))
            for slot, step in zip(slots, (1, -1, 2)):
                yield
                there = dict(here, **{axis: lax.rem(here[axis] + step + 4, 4)})
                copies.wait_recv(
                    slot, region(have, there, core, pl.ds(0, 2)), place.move(axis, step)
                )
        else:
            at = {s: dict(here, **{axis: lax.rem(here[axis] + s + 4, 4)}) for s in (-1, 1, 2)}
            up, down, up2, down2 = (copies.slot() for _ in range(4))
            ahead, behind = place.move(axis, 1), place.move(axis, -1)
            copies.send(up, region(have, here, core, pl.ds(0, 2)), ahead)
            copies.send(down, region(have, here, core, pl.ds(0, 2)), behind)
            yield
            copies.wait_recv(up, region(have, at[-1], core, pl.ds(0, 2)), behind)
            copies.send(up2, region(have, at[-1], core, pl.ds(0, 1)), ahead)
            if last:
                share(have, at[-1])
            yield
            copies.wait_recv(down, region(have, at[1], core, pl.ds(0, 2)), ahead)
            copies.send(down2, region(have, at[1], core, pl.ds(1, 1)), behind)
            if last:
                share(have, at[1])
            yield
            copies.wait_recv(up2, region(have, at[2], core, pl.ds(0, 1)), behind)
            yield
            copies.wait_recv(down2, region(have, at[2], core, pl.ds(1, 1)), ahead)
            if last:
                share(have, at[2])
        have = have + (axis,)
    for slot, ref in from_partner:
        yield
        copies.wait_recv(slot, ref, partner)


GATHER_WALKS = (
    (0, 0, 256, ('y', 'x', 'z')),
    (0, 256, 256, ('x', 'y', 'z')),
    (0, 512, 256, ('z', 'x', 'y')),
    (1, 0, 256, ('y', 'x', 'z')),
    (1, 256, 256, ('x', 'y', 'z')),
    (1, 512, 256, ('y', 'z', 'x')),
    (2, 0, 256, ('y', 'x', 'z')),
    (2, 256, 256, ('z', 'y', 'x')),
    (2, 512, 256, ('z', 'x', 'y')),
    (3, 0, 256, ('z', 'x', 'y')),
    (3, 256, 256, ('x', 'z', 'y')),
    (3, 512, 256, ('y', 'x', 'z')),
    (4, 0, 512, ('y', 'z', 'x')),
    (5, 0, 512, ('y', 'x', 'z')),
    (6, 0, 512, ('x', 'z', 'y')),
    (7, 0, 512, ('y', 'z', 'x')),
)
REDUCE_WALKS = (
    (0, None, ('z', 'y', 'x')),
    (1, None, ('z', 'y', 'x')),
    (2, None, ('z', 'x', 'y')),
    (3, None, ('x', 'z', 'y')),
    (4, 0, ('x', 'z', 'y')),
    (4, 1, ('y', 'z', 'x')),
)
COPIES = 298
SCHEDULE = (
    ('s', 2), ('s', 3), ('e',), ('w', 0), ('w', 1), ('w', 2), ('w', 3), ('w', 4), ('w', 5),
    ('w', 6), ('w', 7), ('w', 8), ('w', 9), ('n', 0), ('n', 1), ('n', 2), ('w', 0), ('w', 0),
    ('w', 1), ('w', 1), ('w', 2), ('w', 2), ('w', 3), ('w', 4), ('n', 3), ('w', 5), ('w', 6),
    ('w', 7), ('w', 7), ('w', 8), ('w', 8), ('w', 9), ('w', 9), ('w', 0), ('w', 3), ('w', 4),
    ('w', 1), ('t', 0), ('w', 2), ('w', 2), ('w', 3), ('w', 4), ('w', 5), ('w', 5), ('w', 6),
    ('w', 8), ('w', 8), ('t', 1), ('w', 0), ('w', 0), ('w', 1), ('w', 1), ('w', 2), ('w', 2),
    ('w', 5), ('w', 5), ('w', 6), ('w', 7), ('w', 7), ('w', 9), ('w', 9), ('w', 4), ('w', 4),
    ('s', 0), ('w', 3), ('w', 3), ('w', 8), ('w', 8), ('s', 1), ('w', 0), ('w', 0), ('w', 1),
    ('w', 1), ('w', 2), ('w', 2), ('w', 5), ('w', 5), ('w', 7), ('w', 7), ('w', 4), ('w', 4),
    ('w', 6), ('w', 6), ('w', 9), ('w', 9), ('s', 4), ('w', 0), ('w', 0), ('w', 0), ('w', 3),
    ('w', 3), ('s', 5), ('w', 5), ('w', 8), ('w', 8), ('w', 5), ('w', 5), ('w', 5), ('w', 5),
    ('s', 6), ('w', 0), ('w', 1), ('w', 1), ('w', 1), ('w', 2), ('w', 2), ('w', 2), ('w', 2),
    ('w', 2), ('w', 10), ('s', 7), ('w', 5), ('w', 7), ('w', 7), ('w', 11), ('w', 6), ('w', 6),
    ('w', 9), ('w', 9), ('w', 10), ('w', 10), ('w', 1), ('w', 12), ('w', 4), ('w', 4), ('w', 4),
    ('w', 2), ('w', 13), ('q', 0), ('w', 8), ('w', 8), ('w', 8), ('w', 8), ('w', 8), ('w', 10),
    ('w', 11), ('w', 11), ('w', 7), ('a', 0, 0), ('w', 3), ('w', 3), ('w', 3), ('w', 4), ('w', 7),
    ('w', 7), ('w', 7), ('w', 7), ('w', 9), ('w', 9), ('w', 9), ('w', 9), ('w', 9), ('w', 11),
    ('w', 12), ('w', 14), ('a', 0, 1), ('w', 8), ('w', 12), ('w', 13), ('w', 15), ('a', 0, 2),
    ('w', 3), ('w', 6), ('w', 6), ('w', 6), ('w', 7), ('w', 10), ('w', 10), ('w', 12), ('w', 13),
    ('w', 9), ('a', 0, 3), ('w', 11), ('w', 11), ('w', 14), ('w', 14), ('w', 15), ('q', 1),
    ('w', 6), ('w', 13), ('w', 15), ('a', 1, 0), ('w', 11), ('w', 11), ('w', 12), ('w', 12),
    ('w', 14), ('w', 15), ('a', 1, 1), ('w', 10), ('w', 10), ('a', 1, 2), ('a', 1, 3), ('w', 13),
    ('w', 13), ('q', 2), ('w', 10), ('w', 10), ('w', 10), ('w', 10), ('w', 10), ('w', 11),
    ('w', 11), ('w', 11), ('a', 2, 0), ('w', 14), ('w', 14), ('a', 2, 1), ('w', 10), ('w', 15),
    ('w', 15), ('a', 2, 2), ('w', 11), ('w', 12), ('w', 12), ('a', 2, 3), ('w', 13), ('w', 13),
    ('q', 3), ('a', 3, 0), ('a', 3, 1), ('w', 14), ('w', 14), ('a', 3, 2), ('w', 15), ('w', 15),
    ('a', 3, 3), ('p', 0), ('p', 1), ('w', 12), ('w', 12), ('w', 12), ('w', 12), ('w', 12),
    ('w', 13), ('w', 13), ('w', 13), ('w', 14), ('w', 14), ('w', 14), ('w', 14), ('w', 14),
    ('p', 2), ('p', 3), ('w', 15), ('w', 15), ('w', 15), ('w', 15), ('w', 15), ('w', 12), ('f', 0),
    ('m', 0), ('w', 16), ('w', 13), ('w', 14), ('w', 15), ('f', 1), ('m', 1), ('w', 17), ('f', 2),
    ('m', 2), ('w', 18), ('w', 16), ('f', 3), ('w', 17), ('m', 3), ('w', 19), ('w', 18), ('w', 16),
    ('w', 16), ('b', 0), ('b', 1), ('w', 16), ('w', 16), ('w', 19), ('b', 2), ('w', 17), ('w', 17),
    ('b', 3), ('w', 17), ('w', 17), ('m', 4), ('w', 20), ('w', 21), ('w', 18), ('w', 18), ('w', 19),
    ('w', 19), ('w', 19), ('w', 19), ('w', 18), ('w', 18), ('w', 20), ('w', 21), ('w', 16),
    ('w', 19), ('w', 16), ('w', 19), ('w', 20), ('w', 20), ('w', 21), ('w', 21), ('w', 17),
    ('w', 17), ('w', 20), ('w', 20), ('w', 21), ('w', 21), ('w', 16), ('w', 16), ('w', 20),
    ('w', 20), ('w', 16), ('w', 16), ('w', 18), ('w', 18), ('w', 19), ('w', 19), ('w', 21),
    ('w', 21), ('w', 19), ('w', 19), ('w', 17), ('w', 17), ('w', 20), ('w', 20), ('w', 20),
    ('w', 20), ('w', 17), ('w', 17), ('w', 18), ('w', 18), ('w', 16), ('w', 16), ('w', 19),
    ('w', 19), ('w', 21), ('w', 21), ('w', 21), ('w', 21), ('w', 18), ('w', 18), ('w', 20),
    ('w', 20), ('w', 17), ('w', 17), ('w', 18), ('w', 18), ('w', 19), ('w', 19), ('w', 16),
    ('w', 16), ('w', 21), ('w', 21), ('w', 20), ('w', 20), ('w', 17), ('w', 17), ('w', 16),
    ('w', 19), ('w', 20), ('w', 18), ('w', 18), ('w', 21), ('w', 21), ('w', 17), ('w', 21),
    ('w', 18),
)


def wide(value):
    return value.astype(jnp.float32)


def reduce_steps(order, table, first_lane, part_of, given, theirs, landing, result, place, copies):
    here = {"x": place.x, "y": place.y, "z": place.z}
    every = pl.ds(0, 2) if part_of is None else pl.ds(part_of, 1)

    def region(done, where, half):
        def pick(axis, extent):
            return pl.ds(where[axis], 1) if axis in done else pl.ds(0, extent)

        zl, lanes = pl.ds(0, 2), pl.ds(first_lane, 256)
        if "z" in done:
            zl = pl.ds(lax.rem(where["z"], 2), 1)
            lanes = pl.ds(pl.multiple_of(first_lane + 128 * lax.div(where["z"], 2), 128), 128)
        if half is None:
            rows = every, pl.ds(0, 2)
        elif part_of is None:
            rows = pl.ds(half, 1), pl.ds(0, 2)
        else:
            rows = every, pl.ds(half, 1)
        return table.at[pick("y", 4), zl, pick("x", 4), *rows, :, lanes]

    partner_slot = copies.slot()
    copies.send(partner_slot, given, place.partner(), dst=theirs)
    yield
    copies.wait_recv(partner_slot, theirs, place.partner())

    def add_partner(y, carry):
        own = table.at[y, :, :, every, :, :, pl.ds(first_lane, 256)]
        own[...] = (wide(own[...]) + wide(theirs[y])).astype(jnp.bfloat16)
        return carry

    lax.fori_loop(0, 4, add_partner, 0)
    done = ()
    for stage, axis in enumerate(order):
        land = landing[stage]
        done = done + (axis,)
        at = {s: dict(here, **{axis: lax.rem(here[axis] + s + 4, 4)}) for s in (-1, 0, 1, 2)}
        ahead, behind = place.move(axis, 1), place.move(axis, -1)
        if stage == 2:
            slots = [copies.slot() for _ in range(3)]
            for slot, step in enumerate((-1, 1, 2)):
                copies.send(
                    slots[slot], region(done, at[step], None), place.move(axis, step), dst=land.at[slot]
                )
            total = wide(region(done, at[0], None)[...])
            for slot, step in enumerate((1, -1, 2)):
                yield
                copies.wait_recv(slots[slot], land.at[slot], place.move(axis, step))
            total = total + wide(land[0]) + wide(land[1]) + wide(land[2])
            count = 64 if part_of is None else 32
            result[pl.ds(0 if part_of is None else 32 * part_of, count), :] = total.reshape(count, 128)
            return
        slots = [copies.slot() for _ in range(6)]

        def send(slot, step, half, peer):
            copies.send(slots[slot], region(done, at[step], half), peer, dst=land.at[slot])

        def wait(slot, peer):
            copies.wait_recv(slots[slot], land.at[slot], peer)

        send(0, 2, 0, ahead)
        send(1, 2, 1, behind)
        send(3, 1, 1, ahead)
        send(4, -1, 0, behind)
        for slot, step, half, source, peer, onward in (
            (0, 1, 0, behind, ahead, 2),
            (1, -1, 1, ahead, behind, 5),
        ):
            yield
            wait(slot, source)
            part = region(done, at[step], half)
            part[...] = (wide(part[...]) + wide(land[slot])).astype(jnp.bfloat16)
            send(onward, step, half, peer)
        for slot, source in ((3, behind), (4, ahead), (2, behind), (5, ahead)):
            yield
            wait(slot, source)
        for half in (0, 1):
            part = region(done, at[0], half)
            total = wide(part[...]) + wide(land[2 + half]) + wide(land[4 + half])
            part[...] = total.astype(jnp.bfloat16)


def stage_shape(unit, part_of, order, stage):
    done = order[: stage + 1]
    x, y = (1 if axis in done else 4 for axis in "xy")
    zl, lanes = (1, 128) if "z" in done else (2, 256)
    if stage == 2:
        return (3, y, zl, x, 2 if part_of is None else 1, 2, 16, lanes)
    return (6, y, zl, x, 1, 2 if part_of is None else 1, 16, lanes)


def wrap32(value):
    value &= 0xFFFFFFFF
    return value - (1 << 32) if value >= 1 << 31 else value


MIX = 747796405


def fill_signs(dst, seed, code, table_columns, first_row, row_total, first_column, spread):
    width = dst.shape[1]
    step = 32
    lanes = lax.broadcasted_iota(jnp.int32, (step, width), 1)
    if spread:
        lanes = lanes + lax.div(lanes, 128) * 384
    tile = (lax.broadcasted_iota(jnp.int32, (step, width), 0) * table_columns + lanes) * MIX
    base = seed * 1664525 + wrap32(code * 374761393 + first_column * MIX)

    def one(i, carry):
        row = first_row + i * step
        hashed = tile + (base + row * wrap32(table_columns * MIX))
        hashed = hashed ^ lax.shift_right_logical(hashed, jnp.int32(15))
        hashed = hashed * 668265261
        hashed = hashed ^ lax.shift_right_logical(hashed, jnp.int32(13))
        hashed = hashed * 1274126177
        hashed = hashed ^ lax.shift_right_logical(hashed, jnp.int32(16))
        signs = jnp.where((hashed & 1) == 1, jnp.float32(1.0), jnp.float32(-1.0))
        dst[pl.ds(pl.multiple_of(row, step), step), :] = signs.astype(jnp.bfloat16)
        return carry

    lax.fori_loop(0, row_total // step, one, 0)


def dot(a, b):
    return jnp.dot(a, b, preferred_element_type=jnp.float32)


def dot_t(a, b):
    return lax.dot_general(a, b, (((1,), (1,)), ((), ())), preferred_element_type=jnp.float32)


def whole_kernel(
    seed_ref, gain, turns, hidden, wq, wk, wv, wo, value_ref, out_ref,
    qkv, out, normed, normed_t, signs, tangent, query, key, value, weights, context, context_t,
    tangent_context, part, cotangent, back_value, theirs, *rest,
):
    landing, (send_sems, recv_sems, load_sems) = rest[:-3], rest[-3:]
    place = Place()
    greet(place)
    bf16 = jnp.bfloat16
    loads = []

    def load(src, dst):
        copy = pltpu.make_async_copy(src, dst, load_sems.at[len(loads)])
        copy.start()
        loads.append(copy)

    def own(buf, columns):
        return buf.at[place.y, place.zl, place.x, place.c, :, :, columns]

    def rows(w, columns):
        return w.at[place.c, :, :, columns]

    load(hidden, normed)
    for h in range(4):
        load(rows(wq, pl.ds(h * 512, 512)), own(qkv.at[h], pl.ds(0, 512)))
        load(rows(wk, pl.ds(h * 128, 128)), own(qkv.at[h], pl.ds(512, 128)))
        load(rows(wv, pl.ds(h * 128, 128)), own(qkv.at[h], pl.ds(640, 128)))
    for j in range(4):
        for p in range(4):
            load(rows(wo, pl.ds(512 * p + 128 * j, 128)), own(out.at[j], pl.ds(128 * p, 128)))
    copies = Copies(send_sems, recv_sems)
    seed = seed_ref[0]

    def enter():
        for copy in loads:
            copy.wait()
        meet(place)

    def norm(i):
        at = pl.ds(128 * i, 128)
        x = normed[at, :].astype(jnp.float32)
        inverse = lax.rsqrt(jnp.mean(x * x, axis=1, keepdims=True) + norm_eps)
        n = (x * inverse * gain[...][None, :].astype(jnp.float32)).astype(bf16)
        normed[at, :] = n
        normed_t[:, at] = n.T

    def tangents(i):
        table = signs.at[0, :, pl.ds(256 * i, 256)]
        fill_signs(table, seed, 0, 512, 0, 2048, 256 * i, False)
        tangent[:, pl.ds(256 * i, 256)] = (dot(normed[...], table[...]) * 2048**-0.5).astype(bf16)

    def sign_part(i):
        fill_signs(signs.at[i // 2], seed, 1, 2048, 1024 * (i % 2), 1024, 128 * (i // 2), True)

    def project(h):
        cosine = jnp.concatenate([turns[0], turns[0]], 0)
        sine = jnp.concatenate([turns[1], turns[1]], 0)

        def rope(x):
            return (x * cosine + pltpu.roll(x, 64, 1) * sine).astype(bf16)

        for block in range(3):
            table = qkv[h, :, :, :, :, :, :, pl.ds(256 * block, 256)].reshape(2048, 256)
            raw = dot(normed[...], table)
            left, right = raw[:, :128], raw[:, 128:]
            if block < 2:
                query[2 * block] = rope(left)
                query[2 * block + 1] = rope(right)
            else:
                key[...] = rope(left)
                value[:, pl.ds(0, 128)] = right.astype(bf16)
                value[:, pl.ds(128, 128)] = tangent[:, pl.ds(128 * h, 128)]

    def attend(h, g):
        causal = lax.broadcasted_iota(jnp.int32, (SEQ, SEQ), 0) >= lax.broadcasted_iota(
            jnp.int32, (SEQ, SEQ), 1
        )
        head = pl.ds(128 * (4 * h + g), 128)
        for s in range(2):
            at = pl.ds(SEQ * s, SEQ)
            scores = dot_t(query[g, at, :], key[at, :]) * HEAD_DIM**-0.5
            scores = jnp.where(causal, scores, -1e30)
            raised = jnp.exp(scores - jnp.max(scores, axis=1, keepdims=True))
            chances = (raised * (1.0 / jnp.sum(raised, axis=1, keepdims=True))).astype(bf16)
            weights[h, s, g] = chances
            mixed = dot(chances, value[at, :]).astype(bf16)
            context[at, head] = mixed[:, :128]
            tangent_context[at, head] = mixed[:, 128:]
            context_t[head, at] = mixed[:, :128].T

    def probe(j):
        def one(block, carry):
            at = pl.ds(pl.multiple_of(256 * block, 256), 256)
            part[j, :, at] = (dot(context[...], signs[j, :, at]) * 2048**-0.5).astype(bf16)
            return carry

        lax.fori_loop(0, 2, one, 0)

    def forward(j):
        def one(block, carry):
            at = pl.ds(pl.multiple_of(256 * block, 256), 256)
            table = out[j, :, :, :, :, :, :, at].reshape(2048, 256)
            total = dot(tangent_context[...], table) + part[j, :, at].astype(jnp.float32)
            cotangent[:, pl.ds(pl.multiple_of(512 * j + 256 * block, 256), 256)] = total.astype(bf16)
            return carry

        lax.fori_loop(0, 2, one, 0)

    def back(h):
        def one(s, carry):
            table = jnp.concatenate([out[j, h].reshape(512, 512) for j in range(4)], 1)
            at = pl.ds(pl.multiple_of(SEQ * s, SEQ), SEQ)
            turned = dot_t(table, cotangent[at, :]).astype(bf16)
            wide_row = jnp.concatenate([turned[128 * g : 128 * g + 128] for g in range(4)], 1)
            spread = dot(wide_row, weights[h, s].reshape(1024, SEQ)).astype(bf16)
            back_value[at, pl.ds(128 * h, 128)] = spread.T
            return carry

        lax.fori_loop(0, 2, one, 0)

    def own_term(unit, zh, core):
        side = lax.rem(place.c + core, 2)
        if unit == 4:
            return side, pl.ds(512 + 128 * zh, 128)
        return unit, pl.ds(pl.multiple_of(256 * side + 128 * zh, 128), 128)

    def terms(unit):
        if unit == TERM_FIRST:
            copies.finish(early_only=True)
        left = normed_t if unit == 4 else context_t

        def one(y, carry):
            rows = left[pl.ds(pl.multiple_of(512 * y, 512), 512), :]
            for zh in range(2):
                if unit == 4:
                    right = back_value[:, pl.ds(256 * zh, 256)]
                else:
                    right = cotangent[:, pl.ds(512 * unit + 256 * zh, 256)]
                both = dot(rows, right).astype(bf16)
                for core in range(2):
                    h, lanes = own_term(unit, zh, core)
                    qkv[h, y, :, :, :, :, :, lanes] = both[:, 128 * core : 128 * core + 128].reshape(
                        2, 4, 2, 2, 16, 128
                    )
            return carry

        lax.fori_loop(0, 4, one, 0)

    def reduce_walk(which):
        unit, part_of, order = REDUCE_WALKS[which]
        mine = (0, 512) if unit == 4 else (unit, 0)
        every = pl.ds(0, 2) if part_of is None else pl.ds(part_of, 1)
        source = (1, 512) if unit == 4 else (unit, 256)
        return reduce_steps(
            order,
            qkv.at[mine[0]],
            mine[1],
            part_of,
            qkv.at[source[0], :, :, :, every, :, :, pl.ds(source[1], 256)],
            theirs.at[unit, :, :, :, every],
            landing[3 * which : 3 * which + 3],
            value_ref if unit == 4 else out_ref.at[:, pl.ds(128 * unit, 128)],
            place,
            copies,
        )

    def gather_walk(chunk, first, columns, order):
        buf = qkv.at[chunk] if chunk < 4 else out.at[chunk - 4]
        return gather_steps(buf, pl.ds(first, columns), order, place, copies)

    gathers = len(GATHER_WALKS)
    walks = [gather_walk(*walk) for walk in GATHER_WALKS]
    walks += [reduce_walk(which) for which in range(len(REDUCE_WALKS))]
    tasks = dict(
        n=norm, t=tangents, s=sign_part, q=project, a=attend, p=probe, f=forward, b=back, m=terms, e=enter
    )
    for what, *where in SCHEDULE:
        if what == "w":
            copies.early = where[0] < gathers and GATHER_WALKS[where[0]][0] < 4
            next(walks[where[0]], None)
        else:
            tasks[what](*where)
    copies.finish()


TERM_FIRST = [where[0] for what, *where in SCHEDULE if what == "m"][0]


def whole(seed, hidden, gain, turns, wq, wk, wv, wo):
    bf16 = jnp.bfloat16
    halves = [w.reshape(2, 2, 16, w.shape[1]) for w in (wq, wk, wv, wo)]
    copies = COPIES
    anywhere = pl.BlockSpec(memory_space=pl.ANY)
    vmem = pl.BlockSpec(memory_space=pltpu.VMEM)
    scratch = [
        (4, 4, 2, 4, 2, 2, 16, 768),
        (4, 4, 2, 4, 2, 2, 16, 512),
        (512, 2048),
        (2048, 512),
        (4, 2048, 512),
        (512, 512),
        (4, 512, 128),
        (512, 128),
        (512, 256),
        (4, 2, 4, SEQ, SEQ),
        (512, 2048),
        (2048, 512),
        (512, 2048),
    ]
    landings = [stage_shape(*walk, stage) for walk in REDUCE_WALKS for stage in range(3)]
    scratch += [(4, 512, 512), (512, 2048), (512, 512), (5, 4, 2, 4, 2, 2, 16, 256)] + landings
    return pl.pallas_call(
        whole_kernel,
        out_shape=[
            jax.ShapeDtypeStruct((64, 128), jnp.float32),
            jax.ShapeDtypeStruct((64, 512), jnp.float32),
        ],
        in_specs=[pl.BlockSpec(memory_space=pltpu.SMEM)] + [vmem] * 2 + [anywhere] * 5,
        out_specs=[vmem] * 2,
        scratch_shapes=[pltpu.VMEM(s, bf16) for s in scratch]
        + [
            pltpu.SemaphoreType.DMA((copies,)),
            pltpu.SemaphoreType.DMA((copies,)),
            pltpu.SemaphoreType.DMA((32,)),
        ],
        compiler_params=pltpu.CompilerParams(
            collective_id=0, has_side_effects=True, vmem_limit_bytes=67043328
        ),
    )(seed, gain, turns, hidden, *halves)


def turn_tables():
    exponent = np.arange(64, dtype=np.float64) * (-2.0 / HEAD_DIM)
    angles = np.arange(SEQ, dtype=np.float64)[:, None] * np.power(rope_base, exponent)[None, :]
    cosine, sine = np.cos(angles), np.sin(angles)
    return np.stack(
        [np.concatenate([cosine, cosine], 1), np.concatenate([-sine, sine], 1)]
    ).astype(np.float32)

def body(hidden, norm_gain, query_weight, key_weight, value_weight, output_weight, probe_seed):
    return tuple(
        whole(
            probe_seed,
            hidden,
            norm_gain,
            jnp.asarray(turn_tables()),
            query_weight,
            key_weight,
            value_weight,
            output_weight,
        )
    )


def solution(mesh):
    return jax.shard_map(
        body,
        mesh=mesh,
        in_specs=(
            P(("probe", "fsdp"), None),
            P(),
            P("fsdp", None),
            P("fsdp", None),
            P("fsdp", None),
            P("fsdp", None),
            P("probe"),
        ),
        out_specs=(P("fsdp", "probe"), P("fsdp", "probe")),
        check_vma=False,
    )
```

```python
import jax
import jax.numpy as jnp
import numpy as np
from jax import lax
from jax.experimental import pallas as pl
from jax.experimental.pallas import tpu as pltpu
from jax.sharding import PartitionSpec as P

MESH = pl.DeviceIdType.MESH
HEAD_DIM = 128
SEQ = 256
norm_eps = 1e-05
rope_base = 500000.0


class Place:
    def __init__(self):
        p = lax.axis_index("probe")
        f = lax.axis_index("fsdp")
        self.p, self.f = p, f
        self.x = lax.rem(f, 4)
        self.zl = lax.rem(lax.div(f, 4), 2)
        self.y = lax.div(f, 8)
        self.zh = lax.div(p, 2)
        self.c = lax.rem(p, 2)
        self.z = self.zh * 2 + self.zl

    def move(self, axis, step):
        x, y, z = self.x, self.y, self.z
        if axis == "x":
            x = lax.rem(x + step + 4, 4)
        elif axis == "y":
            y = lax.rem(y + step + 4, 4)
        else:
            z = lax.rem(z + step + 4, 4)
        return (lax.div(z, 2) * 2 + self.c, y * 8 + lax.rem(z, 2) * 4 + x)

    def partner(self):
        return (self.zh * 2 + 1 - self.c, self.f)

    def neighbours(self):
        return [self.move(a, s) for a in ("x", "y", "z") for s in (1, -1, 2)] + [self.partner()]


def greet(place):
    barrier = pltpu.get_barrier_semaphore()
    for peer in place.neighbours():
        pl.semaphore_signal(barrier, inc=1, device_id=peer, device_id_type=MESH)


def meet(place):
    pl.semaphore_wait(pltpu.get_barrier_semaphore(), len(place.neighbours()))


class Copies:
    def __init__(self, send_sems, recv_sems):
        self.send_sems, self.recv_sems = send_sems, recv_sems
        self.used = 0
        self.early = False
        self.started = []
        self.busy = [None] * SENDS

    def slot(self):
        self.used += 1
        return self.used - 1

    def send(self, slot, ref, peer, dst=None):
        at = len(self.started) % SENDS
        self.release(at)
        copy = pltpu.make_async_remote_copy(
            src_ref=ref,
            dst_ref=ref if dst is None else dst,
            send_sem=self.send_sems.at[at],
            recv_sem=self.recv_sems.at[slot],
            device_id=peer,
            device_id_type=MESH,
        )
        copy.start()
        self.started.append(copy)
        self.busy[at] = (self.early, copy)

    def release(self, at):
        if self.busy[at] is not None:
            self.busy[at][1].wait_send()
            self.busy[at] = None

    def wait_recv(self, slot, ref, peer):
        pltpu.make_async_remote_copy(
            src_ref=ref,
            dst_ref=ref,
            send_sem=self.send_sems.at[0],
            recv_sem=self.recv_sems.at[slot],
            device_id=peer,
            device_id_type=MESH,
        ).wait_recv()

    def finish(self, early_only=False):
        for at in range(SENDS):
            if self.busy[at] is not None and (self.busy[at][0] or not early_only):
                self.release(at)


def gather_steps(buf, lanes, order, place, copies):
    def region(have, where, core, halves, extra=()):
        def pick(axis, extent):
            if axis in extra:
                return pl.ds(0, 3)
            return pl.ds(0, extent) if axis in have else pl.ds(where[axis], 1)

        return buf.at[pick("y", 4), pick("z", 2), pick("x", 4), core, halves, :, lanes]

    here = {"x": place.x, "y": place.y, "z": place.zl}
    core, other, both = place.c, 1 - place.c, pl.ds(0, 2)
    partner = place.partner()
    partner_slot = copies.slot()

    def share(have, where):
        copies.send(partner_slot, region(have, where, core, both), partner)

    have = ()
    for phase, axis in enumerate(order):
        last = phase == 2
        if last:
            share(have, here)
        if axis == "z":
            slot = copies.slot()
            for half, step in ((0, 1), (1, -1)):
                copies.send(slot, region(have, here, core, pl.ds(half, 1)), place.move("z", step))
            there = dict(here, z=1 - place.zl)
            yield
            copies.wait_recv(slot, region(have, there, core, both), place.move("z", 1))
            if last:
                share(have, there)
        elif phase == 0:
            slot = copies.slot()
            for step in (-1, 1, 2):
                copies.send(slot, region(have, here, core, both), place.move(axis, step))
            yield
            copies.wait_recv(slot, region(have, here, core, both, (axis,)), place.move(axis, 1))
        else:
            at = {s: dict(here, **{axis: lax.rem(here[axis] + s + 4, 4)}) for s in (-1, 1, 2)}
            up, down, across = (copies.slot() for _ in range(3))
            ahead, behind = place.move(axis, 1), place.move(axis, -1)
            copies.send(up, region(have, here, core, both), ahead)
            copies.send(down, region(have, here, core, both), behind)
            yield
            copies.wait_recv(up, region(have, at[-1], core, both), behind)
            copies.send(across, region(have, at[-1], core, pl.ds(0, 1)), ahead)
            if last:
                share(have, at[-1])
            yield
            copies.wait_recv(down, region(have, at[1], core, both), ahead)
            copies.send(across, region(have, at[1], core, pl.ds(1, 1)), behind)
            if last:
                share(have, at[1])
            yield
            copies.wait_recv(across, region(have, at[2], core, both), behind)
            if last:
                share(have, at[2])
        have = have + (axis,)
    yield
    copies.wait_recv(partner_slot, region("xyz", here, other, both), partner)


GATHER_WALKS = (
    (0, 0, 256, ('z', 'x', 'y')),
    (0, 256, 256, ('y', 'x', 'z')),
    (0, 512, 256, ('x', 'y', 'z')),
    (1, 0, 256, ('y', 'x', 'z')),
    (1, 256, 256, ('z', 'y', 'x')),
    (1, 512, 256, ('x', 'y', 'z')),
    (2, 0, 256, ('y', 'z', 'x')),
    (2, 256, 256, ('y', 'x', 'z')),
    (2, 512, 256, ('y', 'x', 'z')),
    (3, 0, 256, ('z', 'y', 'x')),
    (3, 256, 256, ('z', 'x', 'y')),
    (3, 512, 256, ('x', 'z', 'y')),
    (4, 0, 512, ('y', 'x', 'z')),
    (5, 0, 512, ('y', 'z', 'x')),
    (6, 0, 512, ('x', 'y', 'z')),
    (7, 0, 512, ('x', 'z', 'y')),
)
REDUCE_WALKS = (
    (0, None, ('z', 'y', 'x')),
    (1, None, ('z', 'x', 'y')),
    (2, None, ('x', 'z', 'y')),
    (3, None, ('y', 'x', 'z')),
    (4, 0, ('z', 'y', 'x')),
    (4, 1, ('y', 'x', 'z')),
)
SENDS = 64
RECEIVES = 168
SCHEDULE = (
    ('s', 2), ('s', 3), ('e',), ('w', 0), ('w', 1), ('w', 2), ('w', 3), ('w', 4), ('w', 5),
    ('w', 6), ('w', 7), ('w', 8), ('w', 9), ('w', 10), ('w', 11), ('n', 0), ('n', 1), ('w', 0),
    ('n', 2), ('n', 3), ('w', 4), ('t', 0), ('w', 1), ('w', 2), ('w', 3), ('w', 5), ('w', 9),
    ('w', 10), ('t', 1), ('w', 0), ('w', 0), ('w', 4), ('w', 4), ('w', 6), ('w', 7), ('w', 8),
    ('w', 11), ('w', 1), ('w', 1), ('s', 0), ('w', 2), ('w', 2), ('w', 3), ('w', 3), ('s', 1),
    ('w', 0), ('w', 5), ('w', 5), ('w', 6), ('w', 10), ('w', 10), ('w', 11), ('w', 9), ('w', 9),
    ('w', 4), ('s', 4), ('w', 2), ('w', 7), ('w', 7), ('s', 5), ('w', 8), ('w', 8), ('s', 6),
    ('w', 1), ('w', 3), ('w', 0), ('w', 0), ('s', 7), ('w', 5), ('w', 2), ('w', 6), ('w', 6),
    ('w', 10), ('w', 11), ('w', 11), ('w', 9), ('w', 1), ('w', 2), ('w', 12), ('w', 0), ('w', 4),
    ('w', 4), ('w', 7), ('w', 8), ('w', 3), ('w', 1), ('w', 13), ('w', 10), ('w', 10), ('w', 0),
    ('w', 6), ('w', 14), ('q', 0), ('w', 5), ('w', 11), ('a', 0, 0), ('w', 3), ('w', 4), ('w', 6),
    ('w', 9), ('w', 9), ('w', 12), ('w', 15), ('a', 0, 1), ('w', 4), ('w', 5), ('w', 7), ('w', 10),
    ('w', 11), ('w', 13), ('w', 14), ('q', 1), ('w', 8), ('w', 9), ('w', 7), ('a', 1, 0), ('w', 10),
    ('w', 12), ('w', 12), ('w', 13), ('a', 1, 1), ('w', 8), ('w', 9), ('w', 14), ('w', 14),
    ('w', 15), ('q', 2), ('w', 12), ('a', 2, 0), ('w', 14), ('w', 15), ('a', 2, 1), ('q', 3),
    ('w', 13), ('w', 13), ('a', 3, 0), ('w', 12), ('a', 3, 1), ('w', 15), ('w', 15), ('p', 0),
    ('w', 13), ('p', 1), ('w', 12), ('f', 0), ('w', 14), ('m', 0), ('w', 16), ('w', 13), ('f', 1),
    ('w', 15), ('m', 1), ('w', 17), ('w', 14), ('p', 2), ('f', 2), ('m', 2), ('w', 18), ('w', 15),
    ('w', 16), ('p', 3), ('f', 3), ('w', 17), ('m', 3), ('w', 19), ('b', 0), ('w', 16), ('w', 16),
    ('w', 18), ('b', 1), ('w', 19), ('b', 2), ('w', 17), ('w', 17), ('w', 18), ('w', 18), ('b', 3),
    ('m', 4), ('w', 20), ('w', 21), ('w', 19), ('w', 19), ('w', 16), ('w', 18), ('w', 17),
    ('w', 20), ('w', 21), ('w', 18), ('w', 18), ('w', 19), ('w', 16), ('w', 16), ('w', 17),
    ('w', 17), ('w', 20), ('w', 20), ('w', 21), ('w', 21), ('w', 19), ('w', 19), ('w', 18),
    ('w', 17), ('w', 16), ('w', 20), ('w', 19), ('w', 21), ('w', 18), ('w', 20), ('w', 20),
    ('w', 21), ('w', 21), ('w', 16), ('w', 17), ('w', 19), ('w', 20), ('w', 21), ('w', 20),
    ('w', 21),
)


def wide(value):
    return value.astype(jnp.float32)


def reduce_steps(order, table, first_lane, part_of, given, theirs, landing, result, place, copies):
    here = {"x": place.x, "y": place.y, "z": place.z}
    every = pl.ds(0, 2) if part_of is None else pl.ds(part_of, 1)

    def region(done, where, half):
        def pick(axis, extent):
            return pl.ds(where[axis], 1) if axis in done else pl.ds(0, extent)

        zl, lanes = pl.ds(0, 2), pl.ds(first_lane, 256)
        if "z" in done:
            zl = pl.ds(lax.rem(where["z"], 2), 1)
            lanes = pl.ds(pl.multiple_of(first_lane + 128 * lax.div(where["z"], 2), 128), 128)
        if half is None:
            rows = every, pl.ds(0, 2)
        elif part_of is None:
            rows = pl.ds(half, 1), pl.ds(0, 2)
        else:
            rows = every, pl.ds(half, 1)
        return table.at[pick("y", 4), zl, pick("x", 4), *rows, :, lanes]

    partner_slot = copies.slot()
    copies.send(partner_slot, given, place.partner(), dst=theirs)
    yield
    copies.wait_recv(partner_slot, theirs, place.partner())

    def add_partner(y, carry):
        own = table.at[y, :, :, every, :, :, pl.ds(first_lane, 256)]
        own[...] = (wide(own[...]) + wide(theirs[y])).astype(jnp.bfloat16)
        return carry

    lax.fori_loop(0, 4, add_partner, 0)
    done = ()
    for stage, axis in enumerate(order):
        land = landing[stage]
        done = done + (axis,)
        at = {s: dict(here, **{axis: lax.rem(here[axis] + s + 4, 4)}) for s in (-1, 0, 1, 2)}
        ahead, behind = place.move(axis, 1), place.move(axis, -1)
        if stage == 2:
            slot = copies.slot()
            for n, step in enumerate((-1, 1, 2)):
                copies.send(slot, region(done, at[step], None), place.move(axis, step), dst=land.at[n])
            total = wide(region(done, at[0], None)[...])
            yield
            copies.wait_recv(slot, land, ahead)
            total = total + wide(land[0]) + wide(land[1]) + wide(land[2])
            count = 64 if part_of is None else 32
            result[pl.ds(0 if part_of is None else 32 * part_of, count), :] = total.reshape(count, 128)
            return
        first, second, rest = (copies.slot() for _ in range(3))

        def send(slot, step, half, peer, to):
            copies.send(slot, region(done, at[step], half), peer, dst=land.at[to])

        send(first, 2, 0, ahead, 0)
        send(second, 2, 1, behind, 1)
        send(rest, 1, 1, ahead, 3)
        send(rest, -1, 0, behind, 4)
        for slot, at_slot, step, half, source, peer, onward in (
            (first, 0, 1, 0, behind, ahead, 2),
            (second, 1, -1, 1, ahead, behind, 5),
        ):
            yield
            copies.wait_recv(slot, land.at[at_slot], source)
            part = region(done, at[step], half)
            part[...] = (wide(part[...]) + wide(land[at_slot])).astype(jnp.bfloat16)
            send(rest, step, half, peer, onward)
        yield
        copies.wait_recv(rest, land.at[pl.ds(2, 4)], behind)
        for half in (0, 1):
            part = region(done, at[0], half)
            total = wide(part[...]) + wide(land[2 + half]) + wide(land[4 + half])
            part[...] = total.astype(jnp.bfloat16)


def stage_shape(unit, part_of, order, stage):
    done = order[: stage + 1]
    x, y = (1 if axis in done else 4 for axis in "xy")
    zl, lanes = (1, 128) if "z" in done else (2, 256)
    if stage == 2:
        return (3, y, zl, x, 2 if part_of is None else 1, 2, 16, lanes)
    return (6, y, zl, x, 1, 2 if part_of is None else 1, 16, lanes)


def wrap32(value):
    value &= 0xFFFFFFFF
    return value - (1 << 32) if value >= 1 << 31 else value


MIX = 747796405


def fill_signs(dst, seed, code, table_columns, first_row, row_total, first_column, spread):
    width = dst.shape[1]
    step = 32
    lanes = lax.broadcasted_iota(jnp.int32, (step, width), 1)
    if spread:
        lanes = lanes + lax.div(lanes, 128) * 384
    tile = (lax.broadcasted_iota(jnp.int32, (step, width), 0) * table_columns + lanes) * MIX
    base = seed * 1664525 + wrap32(code * 374761393 + first_column * MIX)

    def one(i, carry):
        row = first_row + i * step
        hashed = tile + (base + row * wrap32(table_columns * MIX))
        hashed = hashed ^ lax.shift_right_logical(hashed, jnp.int32(15))
        hashed = hashed * 668265261
        hashed = hashed ^ lax.shift_right_logical(hashed, jnp.int32(13))
        hashed = hashed * 1274126177
        hashed = hashed ^ lax.shift_right_logical(hashed, jnp.int32(16))
        signs = jnp.where((hashed & 1) == 1, jnp.float32(1.0), jnp.float32(-1.0))
        dst[pl.ds(pl.multiple_of(row, step), step), :] = signs.astype(jnp.bfloat16)
        return carry

    lax.fori_loop(0, row_total // step, one, 0)


def dot(a, b):
    return jnp.dot(a, b, preferred_element_type=jnp.float32)


def dot_t(a, b):
    return lax.dot_general(a, b, (((1,), (1,)), ((), ())), preferred_element_type=jnp.float32)


def whole_kernel(
    seed_ref, gain, turns, hidden, wq, wk, wv, wo, value_ref, out_ref,
    qkv, out, normed, normed_t, signs, tangent, query, key, value, weights, context, context_t,
    tangent_context, part, cotangent, back_value, theirs, *rest,
):
    landing, (send_sems, recv_sems, load_sems) = rest[:-3], rest[-3:]
    place = Place()
    greet(place)
    bf16 = jnp.bfloat16

    def load(src, dst, sem):
        pltpu.make_async_copy(src, dst, load_sems.at[sem]).start()

    def own(buf, columns):
        return buf.at[place.y, place.zl, place.x, place.c, :, :, columns]

    def rows(w, columns):
        return w.at[place.c, :, :, columns]

    load(hidden, normed, 0)
    for h in range(4):
        load(rows(wq, pl.ds(h * 512, 512)), own(qkv.at[h], pl.ds(0, 512)), 1)
        load(rows(wk, pl.ds(h * 128, 128)), own(qkv.at[h], pl.ds(512, 128)), 1)
        load(rows(wv, pl.ds(h * 128, 128)), own(qkv.at[h], pl.ds(640, 128)), 1)
    for j in range(4):
        for p in range(4):
            load(rows(wo, pl.ds(512 * p + 128 * j, 128)), own(out.at[j], pl.ds(128 * p, 128)), 2)
    copies = Copies(send_sems, recv_sems)
    seed = seed_ref[0]

    def enter():
        pltpu.make_async_copy(hidden, normed, load_sems.at[0]).wait()
        for buf, sem in ((qkv, 1), (out, 2)):
            landed = buf.at[:, place.y, place.zl, place.x, place.c]
            pltpu.make_async_copy(landed, landed, load_sems.at[sem]).wait()
        meet(place)

    def norm(i):
        at = pl.ds(128 * i, 128)
        x = normed[at, :].astype(jnp.float32)
        inverse = lax.rsqrt(jnp.mean(x * x, axis=1, keepdims=True) + norm_eps)
        n = (x * inverse * gain[...][None, :].astype(jnp.float32)).astype(bf16)
        normed[at, :] = n
        normed_t[:, at] = n.T

    def tangents(i):
        table = signs.at[0, :, pl.ds(256 * i, 256)]
        fill_signs(table, seed, 0, 512, 0, 2048, 256 * i, False)
        tangent[:, pl.ds(256 * i, 256)] = (dot(normed[...], table[...]) * 2048**-0.5).astype(bf16)

    def sign_part(i):
        fill_signs(signs.at[i // 2], seed, 1, 2048, 1024 * (i % 2), 1024, 128 * (i // 2), True)

    def project(h):
        cosine = jnp.concatenate([turns[0], turns[0]], 0)
        sine = jnp.concatenate([turns[1], turns[1]], 0)

        def rope(x):
            return (x * cosine + pltpu.roll(x, 64, 1) * sine).astype(bf16)

        for block in range(3):
            table = qkv[h, :, :, :, :, :, :, pl.ds(256 * block, 256)].reshape(2048, 256)
            raw = dot(normed[...], table)
            left, right = raw[:, :128], raw[:, 128:]
            if block < 2:
                query[2 * block] = rope(left)
                query[2 * block + 1] = rope(right)
            else:
                key[...] = rope(left)
                value[:, pl.ds(0, 128)] = right.astype(bf16)
                value[:, pl.ds(128, 128)] = tangent[:, pl.ds(128 * h, 128)]

    def attend(h, pair):
        causal = lax.broadcasted_iota(jnp.int32, (SEQ, SEQ), 0) >= lax.broadcasted_iota(
            jnp.int32, (SEQ, SEQ), 1
        )

        def one(g, carry):
            head = pl.ds(pl.multiple_of(128 * (4 * h + g), 128), 128)
            for s in range(2):
                at = pl.ds(SEQ * s, SEQ)
                scores = dot_t(query[g, at, :], key[at, :]) * HEAD_DIM**-0.5
                scores = jnp.where(causal, scores, -1e30)
                raised = jnp.exp(scores - jnp.max(scores, axis=1, keepdims=True))
                chances = (raised * (1.0 / jnp.sum(raised, axis=1, keepdims=True))).astype(bf16)
                weights[h, s, g] = chances
                mixed = dot(chances, value[at, :]).astype(bf16)
                context[at, head] = mixed[:, :128]
                tangent_context[at, head] = mixed[:, 128:]
                context_t[head, at] = mixed[:, :128].T
            return carry

        lax.fori_loop(2 * pair, 2 * pair + 2, one, 0)

    def probe(j):
        for block in range(2):
            at = pl.ds(256 * block, 256)
            part[j, :, at] = (dot(context[...], signs[j, :, at]) * 2048**-0.5).astype(bf16)

    def forward(j):
        for block in range(2):
            at = pl.ds(256 * block, 256)
            table = out[j, :, :, :, :, :, :, at].reshape(2048, 256)
            total = dot(tangent_context[...], table) + part[j, :, at].astype(jnp.float32)
            cotangent[:, pl.ds(512 * j + 256 * block, 256)] = total.astype(bf16)

    def back(h):
        table = jnp.concatenate([out[j, h].reshape(512, 512) for j in range(4)], 1)
        for s in range(2):
            at = pl.ds(SEQ * s, SEQ)
            turned = dot_t(table, cotangent[at, :]).astype(bf16)
            wide_row = jnp.concatenate([turned[128 * g : 128 * g + 128] for g in range(4)], 1)
            spread = dot(wide_row, weights[h, s].reshape(1024, SEQ)).astype(bf16)
            back_value[at, pl.ds(128 * h, 128)] = spread.T

    def own_term(unit, zh, core):
        side = lax.rem(place.c + core, 2)
        if unit == 4:
            return side, pl.ds(512 + 128 * zh, 128)
        return unit, pl.ds(pl.multiple_of(256 * side + 128 * zh, 128), 128)

    def terms(unit):
        if unit == TERM_FIRST:
            copies.finish(early_only=True)
        left = normed_t if unit == 4 else context_t

        def one(trip, carry):
            for zh in range(2):
                if unit == 4:
                    right = back_value[:, pl.ds(256 * zh, 256)]
                else:
                    right = cotangent[:, pl.ds(512 * unit + 256 * zh, 256)]
                both = dot(left[pl.ds(pl.multiple_of(1024 * trip, 1024), 1024), :], right).astype(bf16)
                for core in range(2):
                    h, lanes = own_term(unit, zh, core)
                    qkv[h, pl.ds(2 * trip, 2), :, :, :, :, :, lanes] = both[
                        :, 128 * core : 128 * core + 128
                    ].reshape(2, 2, 4, 2, 2, 16, 128)
            return carry

        lax.fori_loop(0, 2, one, 0)

    def reduce_walk(which):
        unit, part_of, order = REDUCE_WALKS[which]
        mine = (0, 512) if unit == 4 else (unit, 0)
        every = pl.ds(0, 2) if part_of is None else pl.ds(part_of, 1)
        source = (1, 512) if unit == 4 else (unit, 256)
        return reduce_steps(
            order,
            qkv.at[mine[0]],
            mine[1],
            part_of,
            qkv.at[source[0], :, :, :, every, :, :, pl.ds(source[1], 256)],
            theirs.at[unit, :, :, :, every],
            landing[3 * which : 3 * which + 3],
            value_ref if unit == 4 else out_ref.at[:, pl.ds(128 * unit, 128)],
            place,
            copies,
        )

    def gather_walk(chunk, first, columns, order):
        buf = qkv.at[chunk] if chunk < 4 else out.at[chunk - 4]
        return gather_steps(buf, pl.ds(first, columns), order, place, copies)

    gathers = len(GATHER_WALKS)
    walks = [gather_walk(*walk) for walk in GATHER_WALKS]
    walks += [reduce_walk(which) for which in range(len(REDUCE_WALKS))]
    tasks = dict(
        n=norm, t=tangents, s=sign_part, q=project, a=attend, p=probe, f=forward, b=back, m=terms, e=enter
    )
    for what, *where in SCHEDULE:
        if what == "w":
            copies.early = where[0] < gathers and GATHER_WALKS[where[0]][0] < 4
            next(walks[where[0]], None)
        else:
            tasks[what](*where)
    copies.finish()


TERM_FIRST = [where[0] for what, *where in SCHEDULE if what == "m"][0]


def whole(seed, hidden, gain, turns, wq, wk, wv, wo):
    bf16 = jnp.bfloat16
    halves = [w.reshape(2, 2, 16, w.shape[1]) for w in (wq, wk, wv, wo)]
    anywhere = pl.BlockSpec(memory_space=pl.ANY)
    vmem = pl.BlockSpec(memory_space=pltpu.VMEM)
    scratch = [
        (4, 4, 2, 4, 2, 2, 16, 768),
        (4, 4, 2, 4, 2, 2, 16, 512),
        (512, 2048),
        (2048, 512),
        (4, 2048, 512),
        (512, 512),
        (4, 512, 128),
        (512, 128),
        (512, 256),
        (4, 2, 4, SEQ, SEQ),
        (512, 2048),
        (2048, 512),
        (512, 2048),
    ]
    landings = [stage_shape(*walk, stage) for walk in REDUCE_WALKS for stage in range(3)]
    scratch += [(4, 512, 512), (512, 2048), (512, 512), (5, 4, 2, 4, 2, 2, 16, 256)] + landings
    return pl.pallas_call(
        whole_kernel,
        out_shape=[
            jax.ShapeDtypeStruct((64, 128), jnp.float32),
            jax.ShapeDtypeStruct((64, 512), jnp.float32),
        ],
        in_specs=[pl.BlockSpec(memory_space=pltpu.SMEM)] + [vmem] * 2 + [anywhere] * 5,
        out_specs=[vmem] * 2,
        scratch_shapes=[pltpu.VMEM(s, bf16) for s in scratch]
        + [
            pltpu.SemaphoreType.DMA((SENDS,)),
            pltpu.SemaphoreType.DMA((RECEIVES,)),
            pltpu.SemaphoreType.DMA((3,)),
        ],
        compiler_params=pltpu.CompilerParams(
            collective_id=0, has_side_effects=True, vmem_limit_bytes=67043328
        ),
    )(seed, gain, turns, hidden, *halves)


def turn_tables():
    exponent = np.arange(64, dtype=np.float64) * (-2.0 / HEAD_DIM)
    angles = np.arange(SEQ, dtype=np.float64)[:, None] * np.power(rope_base, exponent)[None, :]
    cosine, sine = np.cos(angles), np.sin(angles)
    return np.stack(
        [np.concatenate([cosine, cosine], 1), np.concatenate([-sine, sine], 1)]
    ).astype(np.float32)

def body(hidden, norm_gain, query_weight, key_weight, value_weight, output_weight, probe_seed):
    return tuple(
        whole(
            probe_seed,
            hidden,
            norm_gain,
            jnp.asarray(turn_tables()),
            query_weight,
            key_weight,
            value_weight,
            output_weight,
        )
    )


def solution(mesh):
    return jax.shard_map(
        body,
        mesh=mesh,
        in_specs=(
            P(("probe", "fsdp"), None),
            P(),
            P("fsdp", None),
            P("fsdp", None),
            P("fsdp", None),
            P("fsdp", None),
            P("probe"),
        ),
        out_specs=(P("fsdp", "probe"), P("fsdp", "probe")),
        check_vma=False,
    )
```

```python
import jax
import jax.numpy as jnp
import numpy as np
from jax import lax
from jax.experimental import pallas as pl
from jax.experimental.pallas import tpu as pltpu
from jax.sharding import PartitionSpec as P

MESH = pl.DeviceIdType.MESH
HEAD_DIM = 128
SEQ = 256
norm_eps = 1e-05
rope_base = 500000.0


class Place:
    def __init__(self):
        p = lax.axis_index("probe")
        f = lax.axis_index("fsdp")
        self.p, self.f = p, f
        self.x = lax.rem(f, 4)
        self.zl = lax.rem(lax.div(f, 4), 2)
        self.y = lax.div(f, 8)
        self.zh = lax.div(p, 2)
        self.c = lax.rem(p, 2)
        self.z = self.zh * 2 + self.zl

    def move(self, axis, step):
        x, y, z = self.x, self.y, self.z
        if axis == "x":
            x = lax.rem(x + step + 4, 4)
        elif axis == "y":
            y = lax.rem(y + step + 4, 4)
        else:
            z = lax.rem(z + step + 4, 4)
        return (lax.div(z, 2) * 2 + self.c, y * 8 + lax.rem(z, 2) * 4 + x)

    def partner(self):
        return (self.zh * 2 + 1 - self.c, self.f)

    def neighbours(self):
        return [self.move(a, s) for a in ("x", "y", "z") for s in (1, -1, 2)] + [self.partner()]


def greet(place):
    barrier = pltpu.get_barrier_semaphore()
    for peer in place.neighbours():
        pl.semaphore_signal(barrier, inc=1, device_id=peer, device_id_type=MESH)


def meet(place):
    pl.semaphore_wait(pltpu.get_barrier_semaphore(), len(place.neighbours()))


class Copies:
    def __init__(self, send_sems, recv_sems):
        self.send_sems, self.recv_sems = send_sems, recv_sems
        self.used = 0
        self.early = False
        self.started = []
        self.busy = [None] * SENDS

    def slot(self):
        self.used += 1
        return self.used - 1

    def send(self, slot, ref, peer, dst=None):
        at = len(self.started) % SENDS
        self.release(at)
        copy = pltpu.make_async_remote_copy(
            src_ref=ref,
            dst_ref=ref if dst is None else dst,
            send_sem=self.send_sems.at[at],
            recv_sem=self.recv_sems.at[slot],
            device_id=peer,
            device_id_type=MESH,
        )
        copy.start()
        self.started.append(copy)
        self.busy[at] = (self.early, copy)

    def release(self, at):
        if self.busy[at] is not None:
            self.busy[at][1].wait_send()
            self.busy[at] = None

    def wait_recv(self, slot, ref, peer):
        pltpu.make_async_remote_copy(
            src_ref=ref,
            dst_ref=ref,
            send_sem=self.send_sems.at[0],
            recv_sem=self.recv_sems.at[slot],
            device_id=peer,
            device_id_type=MESH,
        ).wait_recv()

    def finish(self, early_only=False):
        for at in range(SENDS):
            if self.busy[at] is not None and (self.busy[at][0] or not early_only):
                self.release(at)


def gather_steps(buf, lanes, order, place, copies):
    def region(have, where, core, halves, extra=()):
        def pick(axis, extent):
            if axis in extra:
                return pl.ds(0, 3)
            return pl.ds(0, extent) if axis in have else pl.ds(where[axis], 1)

        return buf.at[pick("y", 4), pick("z", 2), pick("x", 4), core, halves, :, lanes]

    here = {"x": place.x, "y": place.y, "z": place.zl}
    core, other, both = place.c, 1 - place.c, pl.ds(0, 2)
    partner = place.partner()
    partner_slot = copies.slot()

    def share(have, where):
        copies.send(partner_slot, region(have, where, core, both), partner)

    have = ()
    for phase, axis in enumerate(order):
        last = phase == 2
        if last:
            share(have, here)
        if axis == "z":
            slot = copies.slot()
            for half, step in ((0, 1), (1, -1)):
                copies.send(slot, region(have, here, core, pl.ds(half, 1)), place.move("z", step))
            there = dict(here, z=1 - place.zl)
            yield
            copies.wait_recv(slot, region(have, there, core, both), place.move("z", 1))
            if last:
                share(have, there)
        elif phase == 0:
            slot = copies.slot()
            for step in (-1, 1, 2):
                copies.send(slot, region(have, here, core, both), place.move(axis, step))
            yield
            copies.wait_recv(slot, region(have, here, core, both, (axis,)), place.move(axis, 1))
        else:
            at = {s: dict(here, **{axis: lax.rem(here[axis] + s + 4, 4)}) for s in (-1, 1, 2)}
            up, down, across = (copies.slot() for _ in range(3))
            ahead, behind = place.move(axis, 1), place.move(axis, -1)
            copies.send(up, region(have, here, core, both), ahead)
            copies.send(down, region(have, here, core, both), behind)
            yield
            copies.wait_recv(up, region(have, at[-1], core, both), behind)
            copies.send(across, region(have, at[-1], core, pl.ds(0, 1)), ahead)
            if last:
                share(have, at[-1])
            yield
            copies.wait_recv(down, region(have, at[1], core, both), ahead)
            copies.send(across, region(have, at[1], core, pl.ds(1, 1)), behind)
            if last:
                share(have, at[1])
            yield
            copies.wait_recv(across, region(have, at[2], core, both), behind)
            if last:
                share(have, at[2])
        have = have + (axis,)
    yield
    copies.wait_recv(partner_slot, region("xyz", here, other, both), partner)


GATHER_WALKS = (
    (0, 0, 256, ('x', 'y', 'z')),
    (0, 256, 256, ('y', 'x', 'z')),
    (0, 512, 256, ('y', 'z', 'x')),
    (1, 0, 256, ('x', 'z', 'y')),
    (1, 256, 256, ('x', 'y', 'z')),
    (1, 512, 256, ('y', 'x', 'z')),
    (2, 0, 256, ('y', 'z', 'x')),
    (2, 256, 256, ('x', 'y', 'z')),
    (2, 512, 256, ('x', 'z', 'y')),
    (3, 0, 256, ('z', 'y', 'x')),
    (3, 256, 256, ('x', 'y', 'z')),
    (3, 512, 256, ('x', 'y', 'z')),
    (4, 0, 512, ('x', 'y', 'z')),
    (5, 0, 512, ('z', 'y', 'x')),
    (6, 0, 512, ('y', 'x', 'z')),
    (7, 0, 512, ('x', 'z', 'y')),
)
REDUCE_WALKS = (
    (0, None, ('x', 'z', 'y')),
    (1, None, ('x', 'y', 'z')),
    (2, None, ('y', 'x', 'z')),
    (3, None, ('z', 'x', 'y')),
    (4, 0, ('x', 'z', 'y')),
    (4, 1, ('z', 'x', 'y')),
)
SENDS = 64
RECEIVES = 164
SCHEDULE = (
    ('s', 2), ('s', 3), ('e',), ('w', 0), ('w', 1), ('w', 2), ('w', 3), ('w', 4), ('w', 5),
    ('w', 6), ('w', 7), ('w', 8), ('w', 9), ('w', 10), ('w', 11), ('n', 1), ('n', 2), ('n', 0),
    ('n', 3), ('t', 0), ('w', 0), ('w', 1), ('w', 2), ('w', 3), ('w', 9), ('t', 1), ('w', 4),
    ('w', 5), ('w', 6), ('w', 7), ('w', 8), ('w', 2), ('w', 0), ('w', 0), ('s', 0), ('w', 3),
    ('w', 9), ('w', 9), ('w', 10), ('s', 5), ('w', 1), ('w', 1), ('w', 4), ('w', 4), ('w', 6),
    ('w', 8), ('w', 11), ('s', 4), ('w', 5), ('w', 5), ('w', 7), ('w', 7), ('s', 7), ('w', 0),
    ('s', 1), ('w', 2), ('w', 2), ('s', 6), ('w', 1), ('w', 3), ('w', 3), ('w', 9), ('w', 10),
    ('w', 10), ('w', 6), ('w', 6), ('w', 4), ('w', 0), ('w', 5), ('w', 2), ('w', 8), ('w', 8),
    ('w', 1), ('w', 0), ('w', 12), ('w', 11), ('w', 11), ('w', 2), ('w', 13), ('w', 9), ('w', 9),
    ('w', 7), ('w', 1), ('w', 14), ('w', 4), ('q', 0), ('w', 3), ('w', 6), ('w', 10), ('a', 0, 0),
    ('w', 4), ('w', 5), ('w', 8), ('w', 9), ('w', 11), ('w', 12), ('w', 13), ('w', 15), ('w', 3),
    ('a', 0, 1), ('w', 6), ('w', 14), ('w', 7), ('w', 5), ('q', 1), ('w', 8), ('w', 9), ('a', 1, 0),
    ('w', 7), ('w', 10), ('w', 12), ('w', 12), ('w', 15), ('a', 1, 1), ('w', 13), ('w', 13),
    ('w', 14), ('w', 14), ('q', 2), ('w', 10), ('w', 11), ('w', 12), ('w', 15), ('a', 2, 1),
    ('w', 13), ('w', 14), ('a', 2, 0), ('w', 11), ('q', 3), ('a', 3, 0), ('a', 3, 1), ('w', 12),
    ('w', 15), ('w', 15), ('p', 3), ('w', 13), ('w', 13), ('p', 1), ('p', 2), ('w', 12), ('p', 0),
    ('w', 15), ('f', 0), ('w', 13), ('w', 14), ('m', 0), ('w', 16), ('w', 15), ('f', 3), ('m', 3),
    ('w', 19), ('w', 13), ('w', 14), ('f', 1), ('m', 1), ('w', 17), ('f', 2), ('w', 16), ('b', 2),
    ('w', 19), ('w', 17), ('b', 3), ('w', 16), ('w', 16), ('m', 2), ('w', 18), ('b', 1), ('w', 19),
    ('w', 19), ('b', 0), ('w', 17), ('w', 17), ('w', 18), ('m', 4), ('w', 20), ('w', 21), ('w', 19),
    ('w', 16), ('w', 20), ('w', 18), ('w', 18), ('w', 21), ('w', 16), ('w', 16), ('w', 17),
    ('w', 19), ('w', 19), ('w', 20), ('w', 20), ('w', 21), ('w', 21), ('w', 18), ('w', 19),
    ('w', 17), ('w', 17), ('w', 16), ('w', 20), ('w', 21), ('w', 18), ('w', 18), ('w', 20),
    ('w', 20), ('w', 17), ('w', 19), ('w', 21), ('w', 21), ('w', 18), ('w', 16), ('w', 20),
    ('w', 21), ('w', 17), ('w', 20), ('w', 18), ('w', 21),
)


def wide(value):
    return value.astype(jnp.float32)


def reduce_steps(order, table, first_lane, part_of, given, theirs, landing, result, place, copies):
    here = {"x": place.x, "y": place.y, "z": place.z}
    every = pl.ds(0, 2) if part_of is None else pl.ds(part_of, 1)

    def region(done, where, half):
        def pick(axis, extent):
            return pl.ds(where[axis], 1) if axis in done else pl.ds(0, extent)

        zl, lanes = pl.ds(0, 2), pl.ds(first_lane, 256)
        if "z" in done:
            zl = pl.ds(lax.rem(where["z"], 2), 1)
            lanes = pl.ds(pl.multiple_of(first_lane + 128 * lax.div(where["z"], 2), 128), 128)
        if half is None:
            rows = every, pl.ds(0, 2)
        elif part_of is None:
            rows = pl.ds(half, 1), pl.ds(0, 2)
        else:
            rows = every, pl.ds(half, 1)
        return table.at[pick("y", 4), zl, pick("x", 4), *rows, :, lanes]

    partner_slot = copies.slot()
    copies.send(partner_slot, given, place.partner(), dst=theirs)
    yield
    copies.wait_recv(partner_slot, theirs, place.partner())

    def add_partner(y, carry):
        own = table.at[y, :, :, every, :, :, pl.ds(first_lane, 256)]
        own[...] = (wide(own[...]) + wide(theirs[y])).astype(jnp.bfloat16)
        return carry

    lax.fori_loop(0, 4, add_partner, 0)
    done = ()
    for stage, axis in enumerate(order):
        land = landing[stage]
        done = done + (axis,)
        at = {s: dict(here, **{axis: lax.rem(here[axis] + s + 4, 4)}) for s in (-1, 0, 1, 2)}
        ahead, behind = place.move(axis, 1), place.move(axis, -1)
        if stage == 2:
            slot = copies.slot()
            for n, step in enumerate((-1, 1, 2)):
                copies.send(slot, region(done, at[step], None), place.move(axis, step), dst=land.at[n])
            total = wide(region(done, at[0], None)[...])
            yield
            copies.wait_recv(slot, land, ahead)
            total = total + wide(land[0]) + wide(land[1]) + wide(land[2])
            count = 64 if part_of is None else 32
            result[pl.ds(0 if part_of is None else 32 * part_of, count), :] = total.reshape(count, 128)
            return
        first, second, rest = (copies.slot() for _ in range(3))

        def send(slot, step, half, peer, to):
            copies.send(slot, region(done, at[step], half), peer, dst=land.at[to])

        send(first, 2, 0, ahead, 0)
        send(second, 2, 1, behind, 1)
        send(rest, 1, 1, ahead, 3)
        send(rest, -1, 0, behind, 4)
        for slot, at_slot, step, half, source, peer, onward in (
            (first, 0, 1, 0, behind, ahead, 2),
            (second, 1, -1, 1, ahead, behind, 5),
        ):
            yield
            copies.wait_recv(slot, land.at[at_slot], source)
            part = region(done, at[step], half)
            part[...] = (wide(part[...]) + wide(land[at_slot])).astype(jnp.bfloat16)
            send(rest, step, half, peer, onward)
        yield
        copies.wait_recv(rest, land.at[pl.ds(2, 4)], behind)
        for half in (0, 1):
            part = region(done, at[0], half)
            total = wide(part[...]) + wide(land[2 + half]) + wide(land[4 + half])
            part[...] = total.astype(jnp.bfloat16)


def stage_shape(unit, part_of, order, stage):
    done = order[: stage + 1]
    x, y = (1 if axis in done else 4 for axis in "xy")
    zl, lanes = (1, 128) if "z" in done else (2, 256)
    if stage == 2:
        return (3, y, zl, x, 2 if part_of is None else 1, 2, 16, lanes)
    return (6, y, zl, x, 1, 2 if part_of is None else 1, 16, lanes)


def wrap32(value):
    value &= 0xFFFFFFFF
    return value - (1 << 32) if value >= 1 << 31 else value


MIX = 747796405


def fill_signs(dst, seed, code, table_columns, first_row, row_total, first_column, spread):
    width = dst.shape[1]
    step = 32
    lanes = lax.broadcasted_iota(jnp.int32, (step, width), 1)
    if spread:
        lanes = lanes + lax.div(lanes, 128) * 384
    tile = (lax.broadcasted_iota(jnp.int32, (step, width), 0) * table_columns + lanes) * MIX
    base = seed * 1664525 + wrap32(code * 374761393 + first_column * MIX)

    def one(i, carry):
        row = first_row + i * step
        hashed = tile + (base + row * wrap32(table_columns * MIX))
        hashed = hashed ^ lax.shift_right_logical(hashed, jnp.int32(15))
        hashed = hashed * 668265261
        hashed = hashed ^ lax.shift_right_logical(hashed, jnp.int32(13))
        hashed = hashed * 1274126177
        hashed = hashed ^ lax.shift_right_logical(hashed, jnp.int32(16))
        signs = jnp.where((hashed & 1) == 1, jnp.float32(1.0), jnp.float32(-1.0))
        dst[pl.ds(pl.multiple_of(row, step), step), :] = signs.astype(jnp.bfloat16)
        return carry

    lax.fori_loop(0, row_total // step, one, 0)


def dot(a, b):
    return jnp.dot(a, b, preferred_element_type=jnp.float32)


def dot_t(a, b):
    return lax.dot_general(a, b, (((1,), (1,)), ((), ())), preferred_element_type=jnp.float32)


def whole_kernel(
    seed_ref, gain, turns, hidden, wq, wk, wv, wo, result,
    qkv, out, normed, normed_t, signs, tangent, query, key, value, weights, context, context_t,
    tangent_context, part, cotangent, back_value, theirs, *rest,
):
    landing, (send_sems, recv_sems, load_sems) = rest[:-3], rest[-3:]
    place = Place()
    greet(place)
    bf16 = jnp.bfloat16

    def load(src, dst, sem):
        pltpu.make_async_copy(src, dst, load_sems.at[sem]).start()

    def own(buf, columns):
        return buf.at[place.y, place.zl, place.x, place.c, :, :, columns]

    def rows(w, columns):
        return w.at[place.c, :, :, columns]

    load(hidden, normed, 0)
    for h in range(4):
        load(rows(wq, pl.ds(h * 512, 512)), own(qkv.at[h], pl.ds(0, 512)), 1)
        load(rows(wk, pl.ds(h * 128, 128)), own(qkv.at[h], pl.ds(512, 128)), 1)
        load(rows(wv, pl.ds(h * 128, 128)), own(qkv.at[h], pl.ds(640, 128)), 1)
    for j in range(4):
        for p in range(4):
            load(rows(wo, pl.ds(512 * p + 128 * j, 128)), own(out.at[j], pl.ds(128 * p, 128)), 2)
    copies = Copies(send_sems, recv_sems)
    seed = seed_ref[0]

    def enter():
        pltpu.make_async_copy(hidden, normed, load_sems.at[0]).wait()
        for buf, sem in ((qkv, 1), (out, 2)):
            landed = buf.at[:, place.y, place.zl, place.x, place.c]
            pltpu.make_async_copy(landed, landed, load_sems.at[sem]).wait()
        meet(place)

    def norm(i):
        at = pl.ds(128 * i, 128)
        x = normed[at, :].astype(jnp.float32)
        inverse = lax.rsqrt(jnp.mean(x * x, axis=1, keepdims=True) + norm_eps)
        n = (x * inverse * gain[...][None, :].astype(jnp.float32)).astype(bf16)
        normed[at, :] = n
        normed_t[:, at] = n.T

    def tangents(i):
        table = signs.at[0, :, pl.ds(256 * i, 256)]
        fill_signs(table, seed, 0, 512, 0, 2048, 256 * i, False)
        tangent[:, pl.ds(256 * i, 256)] = (dot(normed[...], table[...]) * 2048**-0.5).astype(bf16)

    def sign_part(i):
        fill_signs(signs.at[i // 2], seed, 1, 2048, 1024 * (i % 2), 1024, 128 * (i // 2), True)

    def project(h):
        cosine = jnp.concatenate([turns[0], turns[0]], 0)
        sine = jnp.concatenate([turns[1], turns[1]], 0)

        def rope(x):
            return (x * cosine + pltpu.roll(x, 64, 1) * sine).astype(bf16)

        for block in range(3):
            table = qkv[h, :, :, :, :, :, :, pl.ds(256 * block, 256)].reshape(2048, 256)
            raw = dot(normed[...], table)
            left, right = raw[:, :128], raw[:, 128:]
            if block < 2:
                query[2 * block] = rope(left)
                query[2 * block + 1] = rope(right)
            else:
                key[...] = rope(left)
                value[:, pl.ds(0, 128)] = right.astype(bf16)
                value[:, pl.ds(128, 128)] = tangent[:, pl.ds(128 * h, 128)]

    def attend(h, pair):
        causal = lax.broadcasted_iota(jnp.int32, (SEQ, SEQ), 0) >= lax.broadcasted_iota(
            jnp.int32, (SEQ, SEQ), 1
        )

        def one(g, carry):
            head = pl.ds(pl.multiple_of(128 * (4 * h + g), 128), 128)
            for s in range(2):
                at = pl.ds(SEQ * s, SEQ)
                scores = dot_t(query[g, at, :], key[at, :]) * HEAD_DIM**-0.5
                scores = jnp.where(causal, scores, -1e30)
                raised = jnp.exp(scores - jnp.max(scores, axis=1, keepdims=True))
                chances = (raised * (1.0 / jnp.sum(raised, axis=1, keepdims=True))).astype(bf16)
                weights[h, s, g] = chances
                mixed = dot(chances, value[at, :]).astype(bf16)
                context[at, head] = mixed[:, :128]
                tangent_context[at, head] = mixed[:, 128:]
                context_t[head, at] = mixed[:, :128].T
            return carry

        lax.fori_loop(2 * pair, 2 * pair + 2, one, 0)

    def probe(j):
        for block in range(2):
            at = pl.ds(256 * block, 256)
            part[j, :, at] = (dot(context[...], signs[j, :, at]) * 2048**-0.5).astype(bf16)

    def forward(j):
        for block in range(2):
            at = pl.ds(256 * block, 256)
            table = out[j, :, :, :, :, :, :, at].reshape(2048, 256)
            total = dot(tangent_context[...], table) + part[j, :, at].astype(jnp.float32)
            cotangent[:, pl.ds(512 * j + 256 * block, 256)] = total.astype(bf16)

    def back(h):
        def one(s, carry):
            table = jnp.concatenate([out[j, h].reshape(512, 512) for j in range(4)], 1)
            at = pl.ds(pl.multiple_of(SEQ * s, SEQ), SEQ)
            turned = dot_t(table, cotangent[at, :]).astype(bf16)
            wide_row = jnp.concatenate([turned[128 * g : 128 * g + 128] for g in range(4)], 1)
            spread = dot(wide_row, weights[h, s].reshape(1024, SEQ)).astype(bf16)
            back_value[at, pl.ds(128 * h, 128)] = spread.T
            return carry

        lax.fori_loop(0, 2, one, 0)

    def own_term(unit, zh, core):
        side = lax.rem(place.c + core, 2)
        if unit == 4:
            return side, pl.ds(512 + 128 * zh, 128)
        return unit, pl.ds(pl.multiple_of(256 * side + 128 * zh, 128), 128)

    def terms(unit):
        if unit == TERM_FIRST:
            copies.finish(early_only=True)
        left = normed_t if unit == 4 else context_t

        for zh in range(2):
            if unit == 4:
                right = back_value[:, pl.ds(256 * zh, 256)]
            else:
                right = cotangent[:, pl.ds(512 * unit + 256 * zh, 256)]
            both = dot(left[...], right).astype(bf16)
            for core in range(2):
                h, lanes = own_term(unit, zh, core)
                qkv[h, :, :, :, :, :, :, lanes] = both[:, 128 * core : 128 * core + 128].reshape(
                    4, 2, 4, 2, 2, 16, 128
                )

    def reduce_walk(which):
        unit, part_of, order = REDUCE_WALKS[which]
        mine = (0, 512) if unit == 4 else (unit, 0)
        every = pl.ds(0, 2) if part_of is None else pl.ds(part_of, 1)
        source = (1, 512) if unit == 4 else (unit, 256)
        return reduce_steps(
            order,
            qkv.at[mine[0]],
            mine[1],
            part_of,
            qkv.at[source[0], :, :, :, every, :, :, pl.ds(source[1], 256)],
            theirs.at[unit, :, :, :, every],
            landing[3 * which : 3 * which + 3],
            result.at[:, pl.ds(128 * unit, 128)],
            place,
            copies,
        )

    def gather_walk(chunk, first, columns, order):
        buf = qkv.at[chunk] if chunk < 4 else out.at[chunk - 4]
        return gather_steps(buf, pl.ds(first, columns), order, place, copies)

    gathers = len(GATHER_WALKS)
    walks = [gather_walk(*walk) for walk in GATHER_WALKS]
    walks += [reduce_walk(which) for which in range(len(REDUCE_WALKS))]
    tasks = dict(
        n=norm, t=tangents, s=sign_part, q=project, a=attend, p=probe, f=forward, b=back, m=terms, e=enter
    )
    for what, *where in SCHEDULE:
        if what == "w":
            copies.early = where[0] < gathers and GATHER_WALKS[where[0]][0] < 4
            next(walks[where[0]], None)
        else:
            tasks[what](*where)
    copies.finish()


TERM_FIRST = [where[0] for what, *where in SCHEDULE if what == "m"][0]


def whole(seed, hidden, gain, turns, wq, wk, wv, wo):
    bf16 = jnp.bfloat16
    halves = [w.reshape(2, 2, 16, w.shape[1]) for w in (wq, wk, wv, wo)]
    anywhere = pl.BlockSpec(memory_space=pl.ANY)
    vmem = pl.BlockSpec(memory_space=pltpu.VMEM)
    scratch = [
        (4, 4, 2, 4, 2, 2, 16, 768),
        (4, 4, 2, 4, 2, 2, 16, 512),
        (512, 2048),
        (2048, 512),
        (4, 2048, 512),
        (512, 512),
        (4, 512, 128),
        (512, 128),
        (512, 256),
        (4, 2, 4, SEQ, SEQ),
        (512, 2048),
        (2048, 512),
        (512, 2048),
    ]
    landings = [stage_shape(*walk, stage) for walk in REDUCE_WALKS for stage in range(3)]
    scratch += [(4, 512, 512), (512, 2048), (512, 512), (5, 4, 2, 4, 2, 2, 16, 256)] + landings
    return pl.pallas_call(
        whole_kernel,
        out_shape=jax.ShapeDtypeStruct((64, 640), jnp.float32),
        in_specs=[pl.BlockSpec(memory_space=pltpu.SMEM)] + [vmem] * 2 + [anywhere] * 5,
        out_specs=vmem,
        scratch_shapes=[pltpu.VMEM(s, bf16) for s in scratch]
        + [
            pltpu.SemaphoreType.DMA((SENDS,)),
            pltpu.SemaphoreType.DMA((RECEIVES,)),
            pltpu.SemaphoreType.DMA((3,)),
        ],
        compiler_params=pltpu.CompilerParams(
            collective_id=0, has_side_effects=True, vmem_limit_bytes=67043328
        ),
    )(seed, gain, turns, hidden, *halves)


def turn_tables():
    exponent = np.arange(64, dtype=np.float64) * (-2.0 / HEAD_DIM)
    angles = np.arange(SEQ, dtype=np.float64)[:, None] * np.power(rope_base, exponent)[None, :]
    cosine, sine = np.cos(angles), np.sin(angles)
    return np.stack(
        [np.concatenate([cosine, cosine], 1), np.concatenate([-sine, sine], 1)]
    ).astype(np.float32)

def body(hidden, norm_gain, query_weight, key_weight, value_weight, output_weight, probe_seed):
    both = whole(
        probe_seed,
        hidden,
        norm_gain,
        jnp.asarray(turn_tables()),
        query_weight,
        key_weight,
        value_weight,
        output_weight,
    )
    return both[:, 512:], both[:, :512]


def solution(mesh):
    return jax.shard_map(
        body,
        mesh=mesh,
        in_specs=(
            P(("probe", "fsdp"), None),
            P(),
            P("fsdp", None),
            P("fsdp", None),
            P("fsdp", None),
            P("fsdp", None),
            P("probe"),
        ),
        out_specs=(P("fsdp", "probe"), P("fsdp", "probe")),
        check_vma=False,
    )
```

```python
import jax
import jax.numpy as jnp
import numpy as np
from jax import lax
from jax.experimental import pallas as pl
from jax.experimental.pallas import tpu as pltpu
from jax.sharding import PartitionSpec as P

MESH = pl.DeviceIdType.MESH
HEAD_DIM = 128
SEQ = 256
norm_eps = 1e-05
rope_base = 500000.0


class Place:
    def __init__(self):
        p = lax.axis_index("probe")
        f = lax.axis_index("fsdp")
        self.p, self.f = p, f
        self.x = lax.rem(f, 4)
        self.zl = lax.rem(lax.div(f, 4), 2)
        self.y = lax.div(f, 8)
        self.zh = lax.div(p, 2)
        self.c = lax.rem(p, 2)
        self.z = self.zh * 2 + self.zl

    def move(self, axis, step):
        x, y, z = self.x, self.y, self.z
        if axis == "x":
            x = lax.rem(x + step + 4, 4)
        elif axis == "y":
            y = lax.rem(y + step + 4, 4)
        else:
            z = lax.rem(z + step + 4, 4)
        return (lax.div(z, 2) * 2 + self.c, y * 8 + lax.rem(z, 2) * 4 + x)

    def partner(self):
        return (self.zh * 2 + 1 - self.c, self.f)

    def neighbours(self):
        return [self.move(a, s) for a in ("x", "y", "z") for s in (1, -1, 2)] + [self.partner()]


def greet(place):
    barrier = pltpu.get_barrier_semaphore()
    for peer in place.neighbours():
        pl.semaphore_signal(barrier, inc=1, device_id=peer, device_id_type=MESH)


def meet(place):
    pl.semaphore_wait(pltpu.get_barrier_semaphore(), len(place.neighbours()))


class Copies:
    def __init__(self, send_sems, recv_sems):
        self.send_sems, self.recv_sems = send_sems, recv_sems
        self.used = 0
        self.early = False
        self.started = []
        self.busy = [None] * SENDS

    def slot(self):
        self.used += 1
        return self.used - 1

    def send(self, slot, ref, peer, dst=None):
        at = len(self.started) % SENDS
        self.release(at)
        copy = pltpu.make_async_remote_copy(
            src_ref=ref,
            dst_ref=ref if dst is None else dst,
            send_sem=self.send_sems.at[at],
            recv_sem=self.recv_sems.at[slot],
            device_id=peer,
            device_id_type=MESH,
        )
        copy.start()
        self.started.append(copy)
        self.busy[at] = (self.early, copy)

    def release(self, at):
        if self.busy[at] is not None:
            self.busy[at][1].wait_send()
            self.busy[at] = None

    def wait_recv(self, slot, ref, peer):
        pltpu.make_async_remote_copy(
            src_ref=ref,
            dst_ref=ref,
            send_sem=self.send_sems.at[0],
            recv_sem=self.recv_sems.at[slot],
            device_id=peer,
            device_id_type=MESH,
        ).wait_recv()

    def finish(self, early_only=False):
        for at in range(SENDS):
            if self.busy[at] is not None and (self.busy[at][0] or not early_only):
                self.release(at)


def gather_steps(buf, lanes, order, place, copies):
    def region(have, where, core, halves, extra=()):
        def pick(axis, extent):
            if axis in extra:
                return pl.ds(0, 3)
            return pl.ds(0, extent) if axis in have else pl.ds(where[axis], 1)

        return buf.at[pick("y", 4), pick("z", 2), pick("x", 4), core, halves, :, lanes]

    here = {"x": place.x, "y": place.y, "z": place.zl}
    core, other, both = place.c, 1 - place.c, pl.ds(0, 2)
    partner = place.partner()
    partner_slot = copies.slot()

    def share(have, where):
        copies.send(partner_slot, region(have, where, core, both), partner)

    have = ()
    for phase, axis in enumerate(order):
        last = phase == 2
        if last:
            share(have, here)
        if axis == "z":
            slot = copies.slot()
            for half, step in ((0, 1), (1, -1)):
                copies.send(slot, region(have, here, core, pl.ds(half, 1)), place.move("z", step))
            there = dict(here, z=1 - place.zl)
            yield
            copies.wait_recv(slot, region(have, there, core, both), place.move("z", 1))
            if last:
                share(have, there)
        elif phase == 0:
            slot = copies.slot()
            for step in (-1, 1, 2):
                copies.send(slot, region(have, here, core, both), place.move(axis, step))
            yield
            copies.wait_recv(slot, region(have, here, core, both, (axis,)), place.move(axis, 1))
        else:
            at = {s: dict(here, **{axis: lax.rem(here[axis] + s + 4, 4)}) for s in (-1, 1, 2)}
            up, down, across = (copies.slot() for _ in range(3))
            ahead, behind = place.move(axis, 1), place.move(axis, -1)
            copies.send(up, region(have, here, core, both), ahead)
            copies.send(down, region(have, here, core, both), behind)
            yield
            copies.wait_recv(up, region(have, at[-1], core, both), behind)
            copies.send(across, region(have, at[-1], core, pl.ds(0, 1)), ahead)
            if last:
                share(have, at[-1])
            yield
            copies.wait_recv(down, region(have, at[1], core, both), ahead)
            copies.send(across, region(have, at[1], core, pl.ds(1, 1)), behind)
            if last:
                share(have, at[1])
            yield
            copies.wait_recv(across, region(have, at[2], core, both), behind)
            if last:
                share(have, at[2])
        have = have + (axis,)
    yield
    copies.wait_recv(partner_slot, region("xyz", here, other, both), partner)


GATHER_WALKS = (
    (0, 0, 256, ('x', 'y', 'z')),
    (0, 256, 256, ('y', 'x', 'z')),
    (0, 512, 256, ('y', 'z', 'x')),
    (1, 0, 256, ('x', 'z', 'y')),
    (1, 256, 256, ('x', 'y', 'z')),
    (1, 512, 256, ('y', 'x', 'z')),
    (2, 0, 256, ('y', 'z', 'x')),
    (2, 256, 256, ('x', 'y', 'z')),
    (2, 512, 256, ('x', 'z', 'y')),
    (3, 0, 256, ('z', 'y', 'x')),
    (3, 256, 256, ('x', 'y', 'z')),
    (3, 512, 256, ('x', 'y', 'z')),
    (4, 0, 512, ('x', 'y', 'z')),
    (5, 0, 512, ('z', 'y', 'x')),
    (6, 0, 512, ('y', 'x', 'z')),
    (7, 0, 512, ('x', 'z', 'y')),
)
REDUCE_WALKS = (
    (0, None, ('x', 'z', 'y')),
    (1, None, ('x', 'y', 'z')),
    (2, None, ('y', 'x', 'z')),
    (3, None, ('z', 'x', 'y')),
    (4, 0, ('x', 'z', 'y')),
    (4, 1, ('z', 'x', 'y')),
)
SENDS = 64
RECEIVES = 164
SCHEDULE = (
    ('s', 2), ('s', 3), ('e',), ('w', 0), ('w', 1), ('w', 2), ('w', 3), ('w', 4), ('w', 5),
    ('w', 6), ('w', 7), ('w', 8), ('w', 9), ('w', 10), ('w', 11), ('n', 1), ('n', 2), ('n', 0),
    ('n', 3), ('t', 0), ('w', 0), ('w', 1), ('w', 2), ('w', 3), ('w', 9), ('t', 1), ('w', 4),
    ('w', 5), ('w', 6), ('w', 7), ('w', 8), ('w', 2), ('w', 0), ('w', 0), ('s', 0), ('w', 3),
    ('w', 9), ('w', 9), ('w', 10), ('s', 5), ('w', 1), ('w', 1), ('w', 4), ('w', 4), ('w', 6),
    ('w', 8), ('w', 11), ('s', 4), ('w', 5), ('w', 5), ('w', 7), ('w', 7), ('s', 7), ('w', 0),
    ('s', 1), ('w', 2), ('w', 2), ('s', 6), ('w', 1), ('w', 3), ('w', 3), ('w', 9), ('w', 10),
    ('w', 10), ('w', 6), ('w', 6), ('w', 4), ('w', 0), ('w', 5), ('w', 2), ('w', 8), ('w', 8),
    ('w', 1), ('w', 0), ('w', 12), ('w', 11), ('w', 11), ('w', 2), ('w', 13), ('w', 9), ('w', 9),
    ('w', 7), ('w', 1), ('w', 14), ('w', 4), ('q', 0), ('w', 3), ('w', 6), ('w', 10), ('a', 0, 0),
    ('w', 4), ('w', 5), ('w', 8), ('w', 9), ('w', 11), ('w', 12), ('w', 13), ('w', 15), ('w', 3),
    ('a', 0, 1), ('w', 6), ('w', 14), ('w', 7), ('w', 5), ('q', 1), ('w', 8), ('w', 9), ('a', 1, 0),
    ('w', 7), ('w', 10), ('w', 12), ('w', 12), ('w', 15), ('a', 1, 1), ('w', 13), ('w', 13),
    ('w', 14), ('w', 14), ('q', 2), ('w', 10), ('w', 11), ('w', 12), ('w', 15), ('a', 2, 1),
    ('w', 13), ('w', 14), ('a', 2, 0), ('w', 11), ('q', 3), ('a', 3, 0), ('a', 3, 1), ('w', 12),
    ('w', 15), ('w', 15), ('p', 3), ('w', 13), ('w', 13), ('p', 1), ('p', 2), ('w', 12), ('p', 0),
    ('w', 15), ('f', 0), ('w', 13), ('w', 14), ('m', 0), ('w', 16), ('w', 15), ('f', 3), ('m', 3),
    ('w', 19), ('w', 13), ('w', 14), ('f', 1), ('m', 1), ('w', 17), ('f', 2), ('w', 16), ('b', 2),
    ('w', 19), ('w', 17), ('b', 3), ('w', 16), ('w', 16), ('m', 2), ('w', 18), ('b', 1), ('w', 19),
    ('w', 19), ('b', 0), ('w', 17), ('w', 17), ('w', 18), ('m', 4), ('w', 20), ('w', 21), ('w', 19),
    ('w', 16), ('w', 20), ('w', 18), ('w', 18), ('w', 21), ('w', 16), ('w', 16), ('w', 17),
    ('w', 19), ('w', 19), ('w', 20), ('w', 20), ('w', 21), ('w', 21), ('w', 18), ('w', 19),
    ('w', 17), ('w', 17), ('w', 16), ('w', 20), ('w', 21), ('w', 18), ('w', 18), ('w', 20),
    ('w', 20), ('w', 17), ('w', 19), ('w', 21), ('w', 21), ('w', 18), ('w', 16), ('w', 20),
    ('w', 21), ('w', 17), ('w', 20), ('w', 18), ('w', 21),
)


def wide(value):
    return value.astype(jnp.float32)


def reduce_steps(order, table, first_lane, part_of, given, theirs, landing, result, place, copies):
    here = {"x": place.x, "y": place.y, "z": place.z}
    every = pl.ds(0, 2) if part_of is None else pl.ds(part_of, 1)

    def region(done, where, half):
        def pick(axis, extent):
            return pl.ds(where[axis], 1) if axis in done else pl.ds(0, extent)

        zl, lanes = pl.ds(0, 2), pl.ds(first_lane, 256)
        if "z" in done:
            zl = pl.ds(lax.rem(where["z"], 2), 1)
            lanes = pl.ds(pl.multiple_of(first_lane + 128 * lax.div(where["z"], 2), 128), 128)
        if half is None:
            rows = every, pl.ds(0, 2)
        elif part_of is None:
            rows = pl.ds(half, 1), pl.ds(0, 2)
        else:
            rows = every, pl.ds(half, 1)
        return table.at[pick("y", 4), zl, pick("x", 4), *rows, :, lanes]

    partner_slot = copies.slot()
    copies.send(partner_slot, given, place.partner(), dst=theirs)
    yield
    copies.wait_recv(partner_slot, theirs, place.partner())

    def add_partner(y, carry):
        own = table.at[y, :, :, every, :, :, pl.ds(first_lane, 256)]
        own[...] = (wide(own[...]) + wide(theirs[y])).astype(jnp.bfloat16)
        return carry

    lax.fori_loop(0, 4, add_partner, 0)
    done = ()
    for stage, axis in enumerate(order):
        land = landing[stage]
        done = done + (axis,)
        at = {s: dict(here, **{axis: lax.rem(here[axis] + s + 4, 4)}) for s in (-1, 0, 1, 2)}
        ahead, behind = place.move(axis, 1), place.move(axis, -1)
        if stage == 2:
            slot = copies.slot()
            for n, step in enumerate((-1, 1, 2)):
                copies.send(slot, region(done, at[step], None), place.move(axis, step), dst=land.at[n])
            total = wide(region(done, at[0], None)[...])
            yield
            copies.wait_recv(slot, land, ahead)
            total = total + wide(land[0]) + wide(land[1]) + wide(land[2])
            count = 64 if part_of is None else 32
            result[pl.ds(0 if part_of is None else 32 * part_of, count), :] = total.reshape(count, 128)
            return
        first, second, rest = (copies.slot() for _ in range(3))

        def send(slot, step, half, peer, to):
            copies.send(slot, region(done, at[step], half), peer, dst=land.at[to])

        send(first, 2, 0, ahead, 0)
        send(second, 2, 1, behind, 1)
        send(rest, 1, 1, ahead, 3)
        send(rest, -1, 0, behind, 4)
        for slot, at_slot, step, half, source, peer, onward in (
            (first, 0, 1, 0, behind, ahead, 2),
            (second, 1, -1, 1, ahead, behind, 5),
        ):
            yield
            copies.wait_recv(slot, land.at[at_slot], source)
            part = region(done, at[step], half)
            part[...] = (wide(part[...]) + wide(land[at_slot])).astype(jnp.bfloat16)
            send(rest, step, half, peer, onward)
        yield
        copies.wait_recv(rest, land.at[pl.ds(2, 4)], behind)
        for half in (0, 1):
            part = region(done, at[0], half)
            total = wide(part[...]) + wide(land[2 + half]) + wide(land[4 + half])
            part[...] = total.astype(jnp.bfloat16)


def stage_shape(unit, part_of, order, stage):
    done = order[: stage + 1]
    x, y = (1 if axis in done else 4 for axis in "xy")
    zl, lanes = (1, 128) if "z" in done else (2, 256)
    if stage == 2:
        return (3, y, zl, x, 2 if part_of is None else 1, 2, 16, lanes)
    return (6, y, zl, x, 1, 2 if part_of is None else 1, 16, lanes)


def wrap32(value):
    value &= 0xFFFFFFFF
    return value - (1 << 32) if value >= 1 << 31 else value


MIX = 747796405


def fill_signs(dst, seed, code, table_columns, first_row, row_total, first_column, spread):
    width = dst.shape[1]
    step = 32
    lanes = lax.broadcasted_iota(jnp.int32, (step, width), 1)
    if spread:
        lanes = lanes + lax.div(lanes, 128) * 384
    tile = (lax.broadcasted_iota(jnp.int32, (step, width), 0) * table_columns + lanes) * MIX
    base = seed * 1664525 + wrap32(code * 374761393 + first_column * MIX)

    def one(i, carry):
        row = first_row + i * step
        hashed = tile + (base + row * wrap32(table_columns * MIX))
        hashed = hashed ^ lax.shift_right_logical(hashed, jnp.int32(15))
        hashed = hashed * 668265261
        hashed = hashed ^ lax.shift_right_logical(hashed, jnp.int32(13))
        hashed = hashed * 1274126177
        hashed = hashed ^ lax.shift_right_logical(hashed, jnp.int32(16))
        signs = jnp.where((hashed & 1) == 1, jnp.float32(1.0), jnp.float32(-1.0))
        dst[pl.ds(pl.multiple_of(row, step), step), :] = signs.astype(jnp.bfloat16)
        return carry

    lax.fori_loop(0, row_total // step, one, 0)


def dot(a, b):
    return jnp.dot(a, b, preferred_element_type=jnp.float32)


def dot_t(a, b):
    return lax.dot_general(a, b, (((1,), (1,)), ((), ())), preferred_element_type=jnp.float32)


def whole_kernel(
    seed_ref, gain, turns, hidden, wq, wk, wv, wo, result,
    qkv, out, normed, normed_t, signs, tangent, query, key, value, weights, context, context_t,
    tangent_context, part, cotangent, back_value, theirs, *rest,
):
    landing, (send_sems, recv_sems, load_sems) = rest[:-3], rest[-3:]
    place = Place()
    greet(place)
    bf16 = jnp.bfloat16

    def load(src, dst, sem):
        pltpu.make_async_copy(src, dst, load_sems.at[sem]).start()

    def own(buf, columns):
        return buf.at[place.y, place.zl, place.x, place.c, :, :, columns]

    def rows(w, columns):
        return w.at[place.c, :, :, columns]

    load(hidden, normed, 0)
    for h in range(4):
        load(rows(wq, pl.ds(h * 512, 512)), own(qkv.at[h], pl.ds(0, 512)), 1)
        load(rows(wk, pl.ds(h * 128, 128)), own(qkv.at[h], pl.ds(512, 128)), 1)
        load(rows(wv, pl.ds(h * 128, 128)), own(qkv.at[h], pl.ds(640, 128)), 1)
    for j in range(4):
        for p in range(4):
            load(rows(wo, pl.ds(512 * p + 128 * j, 128)), own(out.at[j], pl.ds(128 * p, 128)), 2)
    copies = Copies(send_sems, recv_sems)
    seed = seed_ref[0]

    def enter():
        pltpu.make_async_copy(hidden, normed, load_sems.at[0]).wait()
        for buf, sem in ((qkv, 1), (out, 2)):
            landed = buf.at[:, place.y, place.zl, place.x, place.c]
            pltpu.make_async_copy(landed, landed, load_sems.at[sem]).wait()
        meet(place)

    def norm(i):
        at = pl.ds(128 * i, 128)
        x = normed[at, :].astype(jnp.float32)
        inverse = lax.rsqrt(jnp.mean(x * x, axis=1, keepdims=True) + norm_eps)
        n = (x * inverse * gain[...][None, :].astype(jnp.float32)).astype(bf16)
        normed[at, :] = n
        normed_t[:, at] = n.T

    def tangents(i):
        table = signs.at[0, :, pl.ds(256 * i, 256)]
        fill_signs(table, seed, 0, 512, 0, 2048, 256 * i, False)
        tangent[:, pl.ds(256 * i, 256)] = (dot(normed[...], table[...]) * 2048**-0.5).astype(bf16)

    def sign_part(i):
        fill_signs(signs.at[i // 2], seed, 1, 2048, 1024 * (i % 2), 1024, 128 * (i // 2), True)

    def project(h):
        cosine = jnp.concatenate([turns[0], turns[0]], 0)
        sine = jnp.concatenate([turns[1], turns[1]], 0)

        def rope(x):
            return (x * cosine + pltpu.roll(x, 64, 1) * sine).astype(bf16)

        for block in range(3):
            table = qkv[h, :, :, :, :, :, :, pl.ds(256 * block, 256)].reshape(2048, 256)
            raw = dot(normed[...], table)
            left, right = raw[:, :128], raw[:, 128:]
            if block < 2:
                query[2 * block] = rope(left)
                query[2 * block + 1] = rope(right)
            else:
                key[...] = rope(left)
                value[:, pl.ds(0, 128)] = right.astype(bf16)
                value[:, pl.ds(128, 128)] = tangent[:, pl.ds(128 * h, 128)]

    def attend(h, pair):
        causal = lax.broadcasted_iota(jnp.int32, (SEQ, SEQ), 0) >= lax.broadcasted_iota(
            jnp.int32, (SEQ, SEQ), 1
        )

        def one(g, carry):
            head = pl.ds(pl.multiple_of(128 * (4 * h + g), 128), 128)
            for s in range(2):
                at = pl.ds(SEQ * s, SEQ)
                scores = dot_t(query[g, at, :], key[at, :]) * HEAD_DIM**-0.5
                scores = jnp.where(causal, scores, -1e30)
                raised = jnp.exp(scores - jnp.max(scores, axis=1, keepdims=True))
                chances = (raised * (1.0 / jnp.sum(raised, axis=1, keepdims=True))).astype(bf16)
                weights[h, s, g] = chances
                mixed = dot(chances, value[at, :]).astype(bf16)
                context[at, head] = mixed[:, :128]
                tangent_context[at, head] = mixed[:, 128:]
                context_t[head, at] = mixed[:, :128].T
            return carry

        lax.fori_loop(2 * pair, 2 * pair + 2, one, 0)

    def probe(j):
        for block in range(2):
            at = pl.ds(256 * block, 256)
            part[j, :, at] = (dot(context[...], signs[j, :, at]) * 2048**-0.5).astype(bf16)

    def forward(j):
        for block in range(2):
            at = pl.ds(256 * block, 256)
            table = out[j, :, :, :, :, :, :, at].reshape(2048, 256)
            total = dot(tangent_context[...], table) + part[j, :, at].astype(jnp.float32)
            cotangent[:, pl.ds(512 * j + 256 * block, 256)] = total.astype(bf16)

    def back(h):
        def one(s, carry):
            table = jnp.concatenate([out[j, h].reshape(512, 512) for j in range(4)], 1)
            at = pl.ds(pl.multiple_of(SEQ * s, SEQ), SEQ)
            turned = dot_t(table, cotangent[at, :]).astype(bf16)
            wide_row = jnp.concatenate([turned[128 * g : 128 * g + 128] for g in range(4)], 1)
            spread = dot(wide_row, weights[h, s].reshape(1024, SEQ)).astype(bf16)
            back_value[at, pl.ds(128 * h, 128)] = spread.T
            return carry

        lax.fori_loop(0, 2, one, 0)

    def own_term(unit, zh, core):
        side = lax.rem(place.c + core, 2)
        if unit == 4:
            return side, pl.ds(512 + 128 * zh, 128)
        return unit, pl.ds(pl.multiple_of(256 * side + 128 * zh, 128), 128)

    def terms(unit):
        if unit == TERM_FIRST:
            copies.finish(early_only=True)
        left = normed_t if unit == 4 else context_t

        for zh in range(2):
            if unit == 4:
                right = back_value[:, pl.ds(256 * zh, 256)]
            else:
                right = cotangent[:, pl.ds(512 * unit + 256 * zh, 256)]
            both = dot(left[...], right).astype(bf16)
            for core in range(2):
                h, lanes = own_term(unit, zh, core)
                qkv[h, :, :, :, :, :, :, lanes] = both[:, 128 * core : 128 * core + 128].reshape(
                    4, 2, 4, 2, 2, 16, 128
                )

    def reduce_walk(which):
        unit, part_of, order = REDUCE_WALKS[which]
        mine = (0, 512) if unit == 4 else (unit, 0)
        every = pl.ds(0, 2) if part_of is None else pl.ds(part_of, 1)
        source = (1, 512) if unit == 4 else (unit, 256)
        return reduce_steps(
            order,
            qkv.at[mine[0]],
            mine[1],
            part_of,
            qkv.at[source[0], :, :, :, every, :, :, pl.ds(source[1], 256)],
            theirs.at[unit, :, :, :, every],
            landing[3 * which : 3 * which + 3],
            result.at[:, pl.ds(128 * unit, 128)],
            place,
            copies,
        )

    def gather_walk(chunk, first, columns, order):
        buf = qkv.at[chunk] if chunk < 4 else out.at[chunk - 4]
        return gather_steps(buf, pl.ds(first, columns), order, place, copies)

    gathers = len(GATHER_WALKS)
    walks = [gather_walk(*walk) for walk in GATHER_WALKS]
    walks += [reduce_walk(which) for which in range(len(REDUCE_WALKS))]
    tasks = dict(
        n=norm, t=tangents, s=sign_part, q=project, a=attend, p=probe, f=forward, b=back, m=terms, e=enter
    )
    for what, *where in SCHEDULE:
        if what == "w":
            copies.early = where[0] < gathers and GATHER_WALKS[where[0]][0] < 4
            next(walks[where[0]], None)
        else:
            tasks[what](*where)
    copies.finish()


TERM_FIRST = [where[0] for what, *where in SCHEDULE if what == "m"][0]


def whole(seed, hidden, gain, turns, wq, wk, wv, wo):
    bf16 = jnp.bfloat16
    halves = [w.reshape(2, 2, 16, w.shape[1]) for w in (wq, wk, wv, wo)]
    anywhere = pl.BlockSpec(memory_space=pl.ANY)
    vmem = pl.BlockSpec(memory_space=pltpu.VMEM)
    scratch = [
        (4, 4, 2, 4, 2, 2, 16, 768),
        (4, 4, 2, 4, 2, 2, 16, 512),
        (512, 2048),
        (2048, 512),
        (4, 2048, 512),
        (512, 512),
        (4, 512, 128),
        (512, 128),
        (512, 256),
        (4, 2, 4, SEQ, SEQ),
        (512, 2048),
        (2048, 512),
        (512, 2048),
    ]
    landings = [stage_shape(*walk, stage) for walk in REDUCE_WALKS for stage in range(3)]
    scratch += [(4, 512, 512), (512, 2048), (512, 512), (5, 4, 2, 4, 2, 2, 16, 256)] + landings
    return pl.pallas_call(
        whole_kernel,
        out_shape=jax.ShapeDtypeStruct((64, 640), jnp.float32),
        in_specs=[pl.BlockSpec(memory_space=pltpu.SMEM)] + [vmem] * 2 + [anywhere] * 5,
        out_specs=vmem,
        scratch_shapes=[pltpu.VMEM(s, bf16) for s in scratch]
        + [
            pltpu.SemaphoreType.DMA((SENDS,)),
            pltpu.SemaphoreType.DMA((RECEIVES,)),
            pltpu.SemaphoreType.DMA((3,)),
        ],
        compiler_params=pltpu.CompilerParams(
            collective_id=0, has_side_effects=True, vmem_limit_bytes=67043328
        ),
    )(seed, gain, turns, hidden, *halves)


def turn_tables():
    exponent = np.arange(64, dtype=np.float64) * (-2.0 / HEAD_DIM)
    angles = np.arange(SEQ, dtype=np.float64)[:, None] * np.power(rope_base, exponent)[None, :]
    cosine, sine = np.cos(angles), np.sin(angles)
    return np.stack(
        [np.concatenate([cosine, cosine], 1), np.concatenate([-sine, sine], 1)]
    ).astype(np.float32)

def part_kernel(both, value_ref, out_ref):
    value_ref[...] = both[:, 512:]
    out_ref[...] = both[:, :512]


def body(hidden, norm_gain, query_weight, key_weight, value_weight, output_weight, probe_seed):
    both = whole(
        probe_seed,
        hidden,
        norm_gain,
        jnp.asarray(turn_tables()),
        query_weight,
        key_weight,
        value_weight,
        output_weight,
    )
    return tuple(
        pl.pallas_call(
            part_kernel,
            out_shape=[
                jax.ShapeDtypeStruct((64, 128), jnp.float32),
                jax.ShapeDtypeStruct((64, 512), jnp.float32),
            ],
        )(both)
    )


def solution(mesh):
    return jax.shard_map(
        body,
        mesh=mesh,
        in_specs=(
            P(("probe", "fsdp"), None),
            P(),
            P("fsdp", None),
            P("fsdp", None),
            P("fsdp", None),
            P("fsdp", None),
            P("probe"),
        ),
        out_specs=(P("fsdp", "probe"), P("fsdp", "probe")),
        check_vma=False,
    )
```
